8 devices in a mesh: rep: 2 (over z, y), dp: 4 (over x, core).
Axes of the slice: x: 2, y: 2, z: 1, core: 2. Of those that a mesh axis runs over, the one named last changes fastest.
Arguments:
- hidden: bfloat16 [512, 7168], P(('rep', 'dp')), parts along dimension 0
- ckv_cache: bfloat16 [512, 512, 512], P(('rep', 'dp')), parts along dimension 0
- kpe_cache: bfloat16 [512, 512, 64], P(('rep', 'dp')), parts along dimension 0
- cache_len: int32 [512], P(('rep', 'dp')), parts along dimension 0
- rope_cos: float32 [512, 32], P(('rep', 'dp')), parts along dimension 0
- rope_sin: float32 [512, 32], P(('rep', 'dp')), parts along dimension 0
- norm_attn: float32 [7168], replicated
- w_dq: bfloat16 [7168, 1536], replicated
- norm_q: float32 [1536], replicated
- w_uq: bfloat16 [1536, 64, 192], replicated
- w_dkv: bfloat16 [7168, 576], replicated
- norm_kv: float32 [512], replicated
- w_uk: bfloat16 [512, 64, 128], replicated
- w_uv: bfloat16 [512, 64, 128], replicated
- w_out: bfloat16 [64, 128, 7168], replicated
- norm_mlp: float32 [7168], replicated
- w_gate: bfloat16 [7168, 18432], P(None, 'dp')
- w_up: bfloat16 [7168, 18432], P(None, 'dp')
- w_down: bfloat16 [18432, 7168], P('dp')
Outputs:
- output 1: bfloat16 [512, 7168], P(('rep', 'dp')), parts along dimension 0
- output 2: bfloat16 [512, 512], P(('rep', 'dp')), parts along dimension 0
- output 3: bfloat16 [512, 64], P(('rep', 'dp')), parts along dimension 0
There are 2 independent parts. The reference program is written for one: setup_inputs(seed, part) draws one part's arguments, and reference() takes and returns one part's arrays. A program takes and returns all parts, laid end to end along the dimension named above; an argument that names none is the same for every part.
All inputs are finite; a program needn't handle non-finite values.
Results may differ from the reference program's by a relative error of at most 0.0108563.
Values are sent between devices in bfloat16 or wider.
A program may use at most 1.75 GiB of HBM per device.

```python
import math
import jax
import jax.numpy as jnp
from jax import lax

BATCH = 256
SEQ_LEN = 512
D_MODEL = 7168
HEADS = 64
Q_LORA = 1536
KV_LORA = 512
NOPE_DIM = 128
ROPE_DIM = 64
V_HEAD = 128
FF_DIM = 18432

EPSILON = 1e-6
MSCALE = 0.1 * math.log(40.0) + 1.0
SCORE_SCALE = MSCALE * MSCALE / math.sqrt(NOPE_DIM + ROPE_DIM)


def weight_draw(rand_key, arr_shape, fan_in):
    return (jax.random.normal(rand_key, arr_shape, jnp.float32) * fan_in ** -0.5).astype(jnp.bfloat16)


def gain_draw(rand_key, vec_size):
    return 1.0 + 0.3 * jax.random.normal(rand_key, (vec_size,), jnp.float32)


def setup_inputs(seed: int = 0, part: int = 0) -> dict:
    base_key = jax.random.key(seed)
    shared_keys = jax.random.split(base_key, 16)
    part_keys = jax.random.split(jax.random.fold_in(base_key, part), 8)
    half_rope = ROPE_DIM // 2
    hidden = jax.random.normal(part_keys[0], (BATCH, D_MODEL), jnp.float32).astype(jnp.bfloat16)
    centre = jax.random.normal(part_keys[1], (BATCH, 1, KV_LORA), jnp.float32)
    spread = jax.random.normal(part_keys[2], (BATCH, SEQ_LEN, KV_LORA), jnp.float32)
    ckv_cache = (0.6 * centre + 0.8 * spread).astype(jnp.bfloat16)
    kpe_cache = jax.random.normal(part_keys[3], (BATCH, SEQ_LEN, ROPE_DIM), jnp.float32).astype(jnp.bfloat16)
    base_len = jax.random.randint(part_keys[4], (BATCH,), 1, SEQ_LEN)
    pick_rows = jax.random.randint(part_keys[5], (2,), 0, BATCH)
    long_row = pick_rows[0]
    short_row = (long_row + 1 + pick_rows[1] % (BATCH - 1)) % BATCH
    cache_len = base_len.at[long_row].set(SEQ_LEN - 1).at[short_row].set(1)
    inv_freq = 10000.0 ** (-jnp.arange(half_rope, dtype=jnp.float32) / half_rope)
    angles = cache_len.astype(jnp.float32)[:, None] * inv_freq[None, :]
    return dict(
        hidden=hidden,
        ckv_cache=ckv_cache,
        kpe_cache=kpe_cache,
        cache_len=cache_len,
        rope_cos=jnp.cos(angles),
        rope_sin=jnp.sin(angles),
        norm_attn=gain_draw(shared_keys[0], D_MODEL),
        w_dq=weight_draw(shared_keys[1], (D_MODEL, Q_LORA), D_MODEL),
        norm_q=gain_draw(shared_keys[2], Q_LORA),
        w_uq=weight_draw(shared_keys[3], (Q_LORA, HEADS, NOPE_DIM + ROPE_DIM), Q_LORA),
        w_dkv=weight_draw(shared_keys[4], (D_MODEL, KV_LORA + ROPE_DIM), D_MODEL),
        norm_kv=gain_draw(shared_keys[5], KV_LORA),
        w_uk=weight_draw(shared_keys[6], (KV_LORA, HEADS, NOPE_DIM), NOPE_DIM),
        w_uv=weight_draw(shared_keys[7], (KV_LORA, HEADS, V_HEAD), KV_LORA),
        w_out=weight_draw(shared_keys[8], (HEADS, V_HEAD, D_MODEL), HEADS * V_HEAD),
        norm_mlp=gain_draw(shared_keys[9], D_MODEL),
        w_gate=weight_draw(shared_keys[10], (D_MODEL, FF_DIM), D_MODEL),
        w_up=weight_draw(shared_keys[11], (D_MODEL, FF_DIM), D_MODEL),
        w_down=weight_draw(shared_keys[12], (FF_DIM, D_MODEL), FF_DIM),
    )


def rms_norm(values_in, gain_vec):
    floats = values_in.astype(jnp.float32)
    mean_sq = jnp.mean(floats * floats, axis=-1, keepdims=True)
    return floats * lax.rsqrt(mean_sq + EPSILON) * gain_vec.astype(jnp.float32)


def apply_rope(values_in, cos_t, sin_t):
    half_dim = values_in.shape[-1] // 2
    low_half = values_in[..., :half_dim]
    high_half = values_in[..., half_dim:]
    return jnp.concatenate([low_half * cos_t - high_half * sin_t, high_half * cos_t + low_half * sin_t], axis=-1)


def one_request(operands):
    q_abs_row, q_pe_row, ckv_row, kpe_row, len_row, ckv_new_row, kpe_new_row = operands
    ckv_float = ckv_row.astype(jnp.float32)
    scores = (jnp.einsum('hl,tl->ht', q_abs_row.astype(jnp.float32), ckv_float)
              + jnp.einsum('hr,tr->ht', q_pe_row.astype(jnp.float32), kpe_row.astype(jnp.float32))) * SCORE_SCALE
    scores = jnp.where(jnp.arange(SEQ_LEN)[None, :] < len_row, scores, -jnp.inf)
    score_new = (jnp.dot(q_abs_row.astype(jnp.float32), ckv_new_row.astype(jnp.float32))
                 + jnp.dot(q_pe_row.astype(jnp.float32), kpe_new_row.astype(jnp.float32))) * SCORE_SCALE
    row_max = jnp.maximum(jnp.max(scores, axis=1), score_new)
    exp_cache = jnp.exp(scores - row_max[:, None])
    exp_new = jnp.exp(score_new - row_max)
    norm_sum = jnp.sum(exp_cache, axis=1) + exp_new
    weighted = (jnp.einsum('ht,tl->hl', exp_cache.astype(jnp.bfloat16).astype(jnp.float32), ckv_float)
                + exp_new.astype(jnp.bfloat16).astype(jnp.float32)[:, None] * ckv_new_row.astype(jnp.float32)[None, :])
    return (weighted / norm_sum[:, None]).astype(jnp.bfloat16)


def reference(hidden, ckv_cache, kpe_cache, cache_len, rope_cos, rope_sin, norm_attn, w_dq, norm_q, w_uq, w_dkv, norm_kv, w_uk, w_uv, w_out, norm_mlp, w_gate, w_up, w_down):
    normed = rms_norm(hidden, norm_attn).astype(jnp.bfloat16)
    q_latent = rms_norm(jnp.dot(normed, w_dq, preferred_element_type=jnp.float32), norm_q).astype(jnp.bfloat16)
    q_full = jnp.einsum('bl,lhe->bhe', q_latent.astype(jnp.float32), w_uq.astype(jnp.float32))
    q_nope = q_full[..., :NOPE_DIM].astype(jnp.bfloat16)
    q_pe = apply_rope(q_full[..., NOPE_DIM:], rope_cos[:, None, :], rope_sin[:, None, :]).astype(jnp.bfloat16)
    kv_full = jnp.dot(normed, w_dkv, preferred_element_type=jnp.float32)
    ckv_new = rms_norm(kv_full[:, :KV_LORA], norm_kv).astype(jnp.bfloat16)
    kpe_new = apply_rope(kv_full[:, KV_LORA:], rope_cos, rope_sin).astype(jnp.bfloat16)
    q_abs = jnp.einsum('bhn,lhn->bhl', q_nope.astype(jnp.float32), w_uk.astype(jnp.float32)).astype(jnp.bfloat16)
    lat_out = lax.map(one_request, (q_abs, q_pe, ckv_cache, kpe_cache, cache_len, ckv_new, kpe_new))
    head_out = jnp.einsum('bhl,lhv->bhv', lat_out.astype(jnp.float32), w_uv.astype(jnp.float32)).astype(jnp.bfloat16)
    attn_out = jnp.einsum('bhv,hvd->bd', head_out.astype(jnp.float32), w_out.astype(jnp.float32))
    residual = (hidden.astype(jnp.float32) + attn_out).astype(jnp.bfloat16)
    mlp_in = rms_norm(residual, norm_mlp).astype(jnp.bfloat16)
    gate_val = jnp.dot(mlp_in, w_gate, preferred_element_type=jnp.float32)
    up_val = jnp.dot(mlp_in, w_up, preferred_element_type=jnp.float32)
    act_val = (jax.nn.silu(gate_val) * up_val).astype(jnp.bfloat16)
    mlp_out = jnp.dot(act_val, w_down, preferred_element_type=jnp.float32)
    out_hidden = (residual.astype(jnp.float32) + mlp_out).astype(jnp.bfloat16)
    return (out_hidden, ckv_new, kpe_new)
```

```python
import math
import jax
import jax.numpy as jnp
from jax import lax
from jax.experimental import pallas as pl
from jax.experimental.pallas import tpu as pltpu
from jax.sharding import PartitionSpec as P

EPSILON = 1e-6
MSCALE = 0.1 * math.log(40.0) + 1.0
MESH = pl.DeviceIdType.MESH


def rms_norm(values_in, gain_vec):
    floats = values_in.astype(jnp.float32)
    mean_sq = jnp.mean(floats * floats, axis=-1, keepdims=True)
    return floats * lax.rsqrt(mean_sq + EPSILON) * gain_vec


def apply_rope(values_in, cos_t, sin_t):
    half_dim = values_in.shape[-1] // 2
    low_half = values_in[..., :half_dim]
    high_half = values_in[..., half_dim:]
    return jnp.concatenate([low_half * cos_t - high_half * sin_t, high_half * cos_t + low_half * sin_t], axis=-1)


def attention_rows(hidden, ckv_cache, kpe_cache, cache_len, rope_cos, rope_sin, norm_attn, w_dq, norm_q, w_uq, w_dkv, norm_kv, w_uk, w_uv):
    nope_dim = w_uk.shape[2]
    value_a7 = w_uk.shape[0]
    score_scale = MSCALE * MSCALE / math.sqrt(w_uq.shape[2])
    normed = rms_norm(hidden, norm_attn).astype(jnp.bfloat16)
    q_latent = rms_norm(jnp.dot(normed, w_dq, preferred_element_type=jnp.float32), norm_q).astype(jnp.bfloat16)
    q_full = jnp.einsum('bl,lhe->bhe', q_latent, w_uq, preferred_element_type=jnp.float32)
    q_nope = q_full[..., :nope_dim].astype(jnp.bfloat16)
    q_pe = apply_rope(q_full[..., nope_dim:], rope_cos[:, None, :], rope_sin[:, None, :]).astype(jnp.bfloat16)
    kv_full = jnp.dot(normed, w_dkv, preferred_element_type=jnp.float32)
    ckv_new = rms_norm(kv_full[:, :value_a7], norm_kv).astype(jnp.bfloat16)
    kpe_new = apply_rope(kv_full[:, value_a7:], rope_cos, rope_sin).astype(jnp.bfloat16)
    q_abs = jnp.einsum('bhn,lhn->bhl', q_nope, w_uk, preferred_element_type=jnp.float32).astype(jnp.bfloat16)
    scores = (jnp.einsum('bhl,btl->bht', q_abs, ckv_cache, preferred_element_type=jnp.float32)
              + jnp.einsum('bhr,btr->bht', q_pe, kpe_cache, preferred_element_type=jnp.float32)) * score_scale
    positions = jnp.arange(ckv_cache.shape[1])
    scores = jnp.where(positions[None, None, :] < cache_len[:, None, None], scores, -jnp.inf)
    score_new = (jnp.einsum('bhl,bl->bh', q_abs, ckv_new, preferred_element_type=jnp.float32)
                 + jnp.einsum('bhr,br->bh', q_pe, kpe_new, preferred_element_type=jnp.float32)) * score_scale
    row_max = jnp.maximum(jnp.max(scores, axis=-1), score_new)
    exp_cache = jnp.exp(scores - row_max[..., None])
    exp_new = jnp.exp(score_new - row_max)
    norm_sum = jnp.sum(exp_cache, axis=-1) + exp_new
    weighted = (jnp.einsum('bht,btl->bhl', exp_cache.astype(jnp.bfloat16), ckv_cache, preferred_element_type=jnp.float32)
                + exp_new.astype(jnp.bfloat16).astype(jnp.float32)[..., None] * ckv_new.astype(jnp.float32)[:, None, :])
    lat_out = (weighted / norm_sum[..., None]).astype(jnp.bfloat16)
    head_out = jnp.einsum('bhl,lhv->bhv', lat_out, w_uv, preferred_element_type=jnp.float32).astype(jnp.bfloat16)
    return head_out, ckv_new, kpe_new


def _sides():
    rep = lax.axis_index('rep')
    me = lax.axis_index('dp')
    chip = me // 2
    core = lax.rem(me, 2)
    return rep, me, chip, core


OUT_W = 512
SLOTS = 4


def tail_kernel(o_ref, x_ref, gain_ref, wout_ref, wgate_ref, wup_ref, wdown_ref, out_ref,
                slots, o_chip, x_chip, r_all, u_all, gate_buf, act, pair_send, pair_recv, far_send, far_recv, own_sum,
                slot_sem, in_send, in_recv, loc_sem, rp_send, rp_recv, rx_send, rx_recv, rf_send, rf_recv,
                pp_send, pp_recv, px_send, px_recv):
    rep, me, chip, core = _sides()
    part = chip * 2 + (1 - core)
    opp = (1 - chip) * 2 + core
    diag = (1 - chip) * 2 + (1 - core)
    attn_k = wout_ref.shape[0]
    d_model = wgate_ref.shape[0]
    ff = wgate_ref.shape[1]
    rows = x_ref.shape[0]
    n_out = d_model // 2 // OUT_W
    n_ff = ff // OUT_W
    n_down = d_model // OUT_W
    first_ff = n_out
    first_down = n_out + 2 * n_ff
    total = first_down + n_down
    half = d_model // 2

    def col(index):
        return pl.ds(pl.multiple_of(index * OUT_W, OUT_W), OUT_W)

    def slot_copy(kind, index, step):
        slot = lax.rem(step, SLOTS)
        src = {'out': wout_ref, 'gate': wgate_ref, 'up': wup_ref, 'down': wdown_ref}[kind]
        depth = src.shape[0]
        return pltpu.make_async_copy(src.at[:, col(index)], slots.at[slot, pl.ds(0, depth), :], slot_sem.at[slot])

    def fetch(step):
        @pl.when(step < first_ff)
        def _():
            slot_copy('out', core * n_out + step, step).start()

        @pl.when((step >= first_ff) & (step < first_down) & (lax.rem(step - first_ff, 2) == 0))
        def _():
            slot_copy('gate', (step - first_ff) // 2, step).start()

        @pl.when((step >= first_ff) & (step < first_down) & (lax.rem(step - first_ff, 2) == 1))
        def _():
            slot_copy('up', (step - first_ff) // 2, step).start()

        @pl.when((step >= first_down) & (step < total))
        def _():
            slot_copy('down', step - first_down, step).start()

    for step in range(SLOTS - 1):
        slot_copy('out', core * n_out + step, step).start()

    barrier = pltpu.get_barrier_semaphore()
    for peer in (part, opp):
        pl.semaphore_signal(barrier, inc=1, device_id=(rep, peer), device_id_type=MESH)
    pl.semaphore_wait(barrier, 2)

    def remote(src, dst, send, recv, peer):
        return pltpu.make_async_remote_copy(src_ref=src, dst_ref=dst, send_sem=send, recv_sem=recv,
                                            device_id=(rep, peer), device_id_type=MESH)

    my_rows = pl.ds(pl.multiple_of(core * rows, rows), rows)
    send_o = remote(o_ref, o_chip.at[my_rows, :], in_send.at[0], in_recv.at[0], part)
    send_o.start()
    their_half = pl.ds(pl.multiple_of((1 - core) * half, half), half)
    send_x = remote(x_ref.at[:, their_half], x_chip.at[my_rows, :], in_send.at[1], in_recv.at[1], part)
    send_x.start()
    my_half = pl.ds(pl.multiple_of(core * half, half), half)
    keep_o = pltpu.make_async_copy(o_ref, o_chip.at[my_rows, :], loc_sem.at[0])
    keep_o.start()
    keep_x = pltpu.make_async_copy(x_ref.at[:, my_half], x_chip.at[my_rows, :], loc_sem.at[1])
    keep_x.start()
    keep_o.wait()
    keep_x.wait()
    send_o.wait()
    send_x.wait()

    chip_rows = pl.ds(pl.multiple_of(chip * 2 * rows, 2 * rows), 2 * rows)
    far_rows = pl.ds(pl.multiple_of((1 - chip) * 2 * rows, 2 * rows), 2 * rows)

    def r_pair(index):
        blk = r_all.at[core * n_out + index, chip_rows, :]
        return remote(blk, blk, rp_send.at[index], rp_recv.at[index], part)

    def r_far(index):
        blk = r_all.at[core * n_out + index, chip_rows, :]
        return remote(blk, blk, rx_send.at[index], rx_recv.at[index], opp)

    def r_forward(index):
        blk = r_all.at[core * n_out + index, far_rows, :]
        return remote(blk, blk, rf_send.at[index], rf_recv.at[index], part)

    def forward(index):
        r_far(index).wait_recv()
        r_forward(index).start()

    def out_step(index, carry):
        fetch(index + SLOTS - 1)
        slot_copy('out', core * n_out + index, index).wait()
        acc = jnp.dot(o_chip[...], slots[lax.rem(index, SLOTS), :attn_k, :], preferred_element_type=jnp.float32)
        r_all[core * n_out + index, chip_rows, :] = (x_chip[:, col(index)].astype(jnp.float32) + acc).astype(jnp.bfloat16)
        r_far(index).start()
        r_pair(index).start()

        @pl.when(index >= 2)
        def _():
            forward(index - 2)
        return carry

    lax.fori_loop(0, n_out, out_step, 0)
    for index in range(n_out - 2, n_out):
        forward(index)
    for index in range(n_out):
        r_pair(index).wait()
        r_far(index).wait_send()
        r_forward(index).wait()

    def square_step(index, total_sq):
        vals = r_all[index].astype(jnp.float32)
        return total_sq + jnp.sum(vals * vals, axis=-1, keepdims=True)

    total_sq = lax.fori_loop(0, n_down, square_step, jnp.zeros((4 * rows, 1), jnp.float32))
    gate_buf[:, 0:1] = lax.rsqrt(total_sq * (1.0 / d_model) + EPSILON)
    order = (part, diag, me, opp)

    def norm_step(index, carry):
        for place, owner in enumerate(order):
            src = pl.ds(pl.multiple_of(owner * rows, rows), rows)
            vals = r_all[index, src, :].astype(jnp.float32) * gate_buf[src, 0:1] * gain_ref[0:1, col(index)]
            u_all[place * rows:(place + 1) * rows, col(index)] = vals.astype(jnp.bfloat16)
        return carry

    lax.fori_loop(0, n_down, norm_step, 0)

    def ff_step(index, carry):
        step = first_ff + 2 * index
        fetch(step + SLOTS - 1)
        slot_copy('gate', index, step).wait()
        gate_buf[...] = jnp.dot(u_all[...], slots[lax.rem(step, SLOTS), :d_model, :], preferred_element_type=jnp.float32)
        fetch(step + SLOTS)
        slot_copy('up', index, step + 1).wait()
        up_val = jnp.dot(u_all[...], slots[lax.rem(step + 1, SLOTS), :d_model, :], preferred_element_type=jnp.float32)
        gate_val = gate_buf[...]
        act[:, col(index)] = (gate_val * jax.nn.sigmoid(gate_val) * up_val).astype(jnp.bfloat16)
        return carry

    lax.fori_loop(0, n_ff, ff_step, 0)

    def pair_copy(index):
        return remote(pair_send.at[index], pair_recv.at[index], pp_send.at[index], pp_recv.at[index], part)

    def far_copy(index):
        return remote(far_send.at[index], far_recv.at[index], px_send.at[index], px_recv.at[index], opp)

    def combine(index):
        pair_copy(index).wait_recv()
        far_send[index] += pair_recv[index, rows:, :]
        far_copy(index).start()
        own_sum[index] += pair_recv[index, :rows, :]

    def down_step(index, carry):
        step = first_down + index
        fetch(step + SLOTS - 1)
        slot_copy('down', index, step).wait()
        part_sum = jnp.dot(act[...], slots[lax.rem(step, SLOTS), :ff, :], preferred_element_type=jnp.float32)
        pair_send[index] = part_sum[:2 * rows]
        own_sum[index] = part_sum[2 * rows:3 * rows]
        far_send[index] = part_sum[3 * rows:]
        pair_copy(index).start()

        @pl.when(index >= 1)
        def _():
            combine(index - 1)
        return carry

    lax.fori_loop(0, n_down, down_step, 0)
    combine(n_down - 1)
    own_rows = pl.ds(pl.multiple_of(me * rows, rows), rows)

    def finish(index, carry):
        far_copy(index).wait()
        pair_copy(index).wait_send()
        mlp = own_sum[index] + far_recv[index]
        out_ref[:, col(index)] = (r_all[index, own_rows, :].astype(jnp.float32) + mlp).astype(jnp.bfloat16)
        return carry

    lax.fori_loop(0, n_down, finish, 0)


def tail(head_out, hidden, norm_mlp, w_out, w_gate, w_up, w_down):
    rows, d_model = hidden.shape
    attn_k = w_out.shape[0]
    ff = w_gate.shape[1]
    n_out = d_model // 2 // OUT_W
    n_down = d_model // OUT_W
    depth = max(attn_k, d_model, ff)
    vmem = pl.BlockSpec(memory_space=pltpu.VMEM)
    anywhere = pl.BlockSpec(memory_space=pl.ANY)
    dma = pltpu.SemaphoreType.DMA
    f32, bf16 = jnp.float32, jnp.bfloat16
    return pl.pallas_call(
        tail_kernel,
        out_shape=jax.ShapeDtypeStruct((rows, d_model), bf16),
        in_specs=[vmem, vmem, vmem, anywhere, anywhere, anywhere, anywhere],
        out_specs=vmem,
        scratch_shapes=[
            pltpu.VMEM((SLOTS, depth, OUT_W), bf16),
            pltpu.VMEM((2 * rows, attn_k), bf16),
            pltpu.VMEM((2 * rows, d_model // 2), bf16),
            pltpu.VMEM((n_down, 4 * rows, OUT_W), bf16),
            pltpu.VMEM((4 * rows, d_model), bf16),
            pltpu.VMEM((4 * rows, OUT_W), f32),
            pltpu.VMEM((4 * rows, ff), bf16),
            pltpu.VMEM((n_down, 2 * rows, OUT_W), f32),
            pltpu.VMEM((n_down, 2 * rows, OUT_W), f32),
            pltpu.VMEM((n_down, rows, OUT_W), f32),
            pltpu.VMEM((n_down, rows, OUT_W), f32),
            pltpu.VMEM((n_down, rows, OUT_W), f32),
            dma((SLOTS,)), dma((2,)), dma((2,)), dma((2,)),
            dma((n_out,)), dma((n_out,)), dma((n_out,)), dma((n_out,)), dma((n_out,)), dma((n_out,)),
            dma((n_down,)), dma((n_down,)), dma((n_down,)), dma((n_down,)),
        ],
        compiler_params=pltpu.CompilerParams(collective_id=0, has_side_effects=True, vmem_limit_bytes=66 * 1000 * 1000),
        name='tail',
    )(head_out, hidden, norm_mlp.reshape(1, d_model), w_out, w_gate, w_up, w_down)


def solution(mesh):
    row_spec = P(('rep', 'dp'), None)
    cube_spec = P(('rep', 'dp'), None, None)
    full_spec = P()
    in_specs = (row_spec, cube_spec, cube_spec, P(('rep', 'dp')), row_spec, row_spec,
                full_spec, full_spec, full_spec, full_spec, full_spec, full_spec, full_spec, full_spec, full_spec, full_spec,
                P(None, 'dp'), P(None, 'dp'), P('dp', None))

    def local_step(hidden, ckv_cache, kpe_cache, cache_len, rope_cos, rope_sin, norm_attn, w_dq, norm_q, w_uq, w_dkv, norm_kv, w_uk, w_uv, w_out, norm_mlp, w_gate, w_up, w_down):
        head_out, ckv_new, kpe_new = attention_rows(hidden, ckv_cache, kpe_cache, cache_len, rope_cos, rope_sin, norm_attn, w_dq, norm_q, w_uq, w_dkv, norm_kv, w_uk, w_uv)
        out_hidden = tail(head_out.reshape(hidden.shape[0], -1), hidden, norm_mlp, w_out.reshape(-1, w_out.shape[-1]), w_gate, w_up, w_down)
        return out_hidden, ckv_new, kpe_new

    return jax.shard_map(local_step, mesh=mesh, in_specs=in_specs, out_specs=(row_spec, row_spec, row_spec), check_vma=False)
```

```python
import functools
import math
import jax
import jax.numpy as jnp
from jax import lax
from jax.experimental import pallas as pl
from jax.experimental.pallas import tpu as pltpu
from jax.sharding import PartitionSpec as P

EPSILON = 1e-6
MSCALE = 0.1 * math.log(40.0) + 1.0
MESH = pl.DeviceIdType.MESH


OUT_W = 512
PIECE = 256
SLOTS = 4
EARLY = 2
HEAD_BLOCK = 8
SWAP_BLOCK = 16
NT = (((1,), (1,)), ((), ()))
NN = (((1,), (0,)), ((), ()))


GROUP = 8
BUFFERS = 3
CHUNK = 128


def attend_kernel(score_scale, len_ref, abs_hbm, pe_hbm, new_ref, pe_new_ref, ckv_ref, kpe_ref, wuv_ref,
                  out_ref, new_out_ref, pe_out_ref, order_buf, turned_buf, abs_ref, pe_ref, kv_buf, kp_buf, lat_buf, wuv_buf, kv_sem, kp_sem, wuv_sem, query_sem):
    query_copies = [pltpu.make_async_copy(abs_hbm, abs_ref, query_sem.at[0]), pltpu.make_async_copy(pe_hbm, pe_ref, query_sem.at[1])]
    for made in query_copies:
        made.start()
    rows, heads, latent_dim = abs_ref.shape
    seq = ckv_ref.shape[1]
    variants = seq // CHUNK
    groups = rows // GROUP
    value_dim = wuv_ref.shape[2]

    def chunks_of(row):
        return len_ref[row] // CHUNK

    def count_step(row, tally):
        return tuple(count + (chunks_of(row) == which).astype(jnp.int32) for which, count in enumerate(tally))

    tally = lax.fori_loop(0, rows, count_step, (jnp.int32(0),) * variants)
    starts = [jnp.int32(0)]
    for which in range(variants - 1):
        starts.append(starts[-1] + tally[which])

    def place_step(row, heads_of):
        mine = [chunks_of(row) == which for which in range(variants)]
        place = sum(jnp.where(hit, head, 0) for hit, head in zip(mine, heads_of))
        order_buf[place] = row
        return tuple(head + hit.astype(jnp.int32) for hit, head in zip(mine, heads_of))

    lax.fori_loop(0, rows, place_step, tuple(starts))

    def group_chunks(group):
        return chunks_of(order_buf[group * GROUP + GROUP - 1]) + 1

    def copies(group, size):
        slot = lax.rem(group, BUFFERS)
        made = []
        for place in range(GROUP):
            row = order_buf[group * GROUP + place]
            made.append(pltpu.make_async_copy(ckv_ref.at[row, pl.ds(0, size), :], kv_buf.at[slot, place, pl.ds(0, size), :], kv_sem.at[slot, place]))
            made.append(pltpu.make_async_copy(kpe_ref.at[row, :, pl.ds(0, size)], kp_buf.at[slot, place, :, pl.ds(0, size)], kp_sem.at[slot, place]))
        return made

    def start(group):
        for count in range(1, variants + 1):
            @pl.when(group_chunks(group) == count)
            def _():
                for made in copies(group, count * CHUNK):
                    made.start()

    for group in range(BUFFERS - 1):
        start(group)
    wuv_copy = pltpu.make_async_copy(wuv_ref, wuv_buf, wuv_sem)
    wuv_copy.start()
    turned_buf[...] = pe_new_ref[...].astype(jnp.float32).T
    new_out_ref[...] = new_ref[...]
    pe_out_ref[...] = pe_new_ref[...]

    def compute(group, size):
        slot = lax.rem(group, BUFFERS)
        for made in copies(group, size):
            made.wait()
        rows_of = [order_buf[group * GROUP + place] for place in range(GROUP)]
        for place, row in enumerate(rows_of):
            length = len_ref[row]
            base = pl.multiple_of((row // 16) * 16, 16)
            picked = new_ref[pl.ds(base, 16), :].astype(jnp.float32)
            hit = lax.broadcasted_iota(jnp.int32, picked.shape, 0) == row - base
            new = jnp.sum(jnp.where(hit, picked, 0.0), axis=0, keepdims=True)
            hit = lax.broadcasted_iota(jnp.int32, turned_buf.shape, 1) == row
            new_pe = jnp.sum(jnp.where(hit, turned_buf[...], 0.0), axis=1, keepdims=True)
            base = pl.multiple_of((length // 16) * 16, 16)
            block = kv_buf[slot, place, pl.ds(base, 16), :]
            hit = lax.broadcasted_iota(jnp.int32, block.shape, 0) == length - base
            kv_buf[slot, place, pl.ds(base, 16), :] = jnp.where(hit, new, block.astype(jnp.float32)).astype(jnp.bfloat16)
            lane = pl.multiple_of((length // CHUNK) * CHUNK, CHUNK)
            block = kp_buf[slot, place, :, pl.ds(lane, CHUNK)]
            hit = lax.broadcasted_iota(jnp.int32, block.shape, 1) == length - lane
            kp_buf[slot, place, :, pl.ds(lane, CHUNK)] = jnp.where(hit, new_pe, block.astype(jnp.float32)).astype(jnp.bfloat16)
        all_scores = [(lax.dot_general(abs_ref[row], kv_buf[slot, place, :size, :], NT, preferred_element_type=jnp.float32)
                       + jnp.dot(pe_ref[row], kp_buf[slot, place, :, :size], preferred_element_type=jnp.float32)) * score_scale
                      for place, row in enumerate(rows_of)]
        weights = []
        for place, row in enumerate(rows_of):
            positions = lax.broadcasted_iota(jnp.int32, (heads, size), 1)
            scores = jnp.where(positions <= len_ref[row], all_scores[place], -jnp.inf)
            exp_all = jnp.exp(scores - jnp.max(scores, axis=1, keepdims=True))
            weights.append((exp_all.astype(jnp.bfloat16), jnp.sum(exp_all, axis=1, keepdims=True)))
        for place, row in enumerate(rows_of):
            weighted = jnp.dot(weights[place][0], kv_buf[slot, place, :size, :], preferred_element_type=jnp.float32)
            lat_buf[row] = (weighted / weights[place][1]).astype(jnp.bfloat16)

    def group_step(group, carry):
        @pl.when(group + BUFFERS - 1 < groups)
        def _():
            start(group + BUFFERS - 1)
        for count in range(1, variants + 1):
            @pl.when(group_chunks(group) == count)
            def _():
                compute(group, count * CHUNK)
        return carry

    for made in query_copies:
        made.wait()
    lax.fori_loop(0, groups, group_step, 0)
    wuv_copy.wait()

    def value_step(block, carry):
        sel = pl.ds(pl.multiple_of(block * SWAP_BLOCK, SWAP_BLOCK), SWAP_BLOCK)
        lat = jnp.swapaxes(lat_buf[:, sel, :], 0, 1)
        wuv = jnp.swapaxes(wuv_buf[:, sel, :], 0, 1)
        for head in range(SWAP_BLOCK):
            dst = pl.ds(pl.multiple_of(block * SWAP_BLOCK * value_dim + head * value_dim, value_dim), value_dim)
            out_ref[:, dst] = jnp.dot(lat[head], wuv[head], preferred_element_type=jnp.float32).astype(jnp.bfloat16)
        return carry

    lax.fori_loop(0, heads // SWAP_BLOCK, value_step, 0)


def attend(q_abs, q_pe, ckv_new, kpe_new, ckv_cache, kpe_cache, cache_len, w_uv, score_scale):
    rows, heads, latent_dim = q_abs.shape
    rope_dim = q_pe.shape[2]
    seq = ckv_cache.shape[1]
    value_dim = w_uv.shape[2]
    smem = pl.BlockSpec(memory_space=pltpu.SMEM)
    vmem = pl.BlockSpec(memory_space=pltpu.VMEM)
    anywhere = pl.BlockSpec(memory_space=pl.ANY)
    dma = pltpu.SemaphoreType.DMA
    return pl.pallas_call(
        functools.partial(attend_kernel, score_scale),
        out_shape=[jax.ShapeDtypeStruct((rows, heads * value_dim), jnp.bfloat16),
                   jax.ShapeDtypeStruct(ckv_new.shape, jnp.bfloat16), jax.ShapeDtypeStruct(kpe_new.shape, jnp.bfloat16)],
        in_specs=[smem, anywhere, anywhere, vmem, vmem, anywhere, anywhere, anywhere],
        out_specs=[vmem, vmem, vmem],
        scratch_shapes=[
            pltpu.SMEM((rows,), jnp.int32),
            pltpu.VMEM((rope_dim, rows), jnp.float32),
            pltpu.VMEM(q_abs.shape, jnp.bfloat16),
            pltpu.VMEM(q_pe.shape, jnp.bfloat16),
            pltpu.VMEM((BUFFERS, GROUP, seq, latent_dim), jnp.bfloat16),
            pltpu.VMEM((BUFFERS, GROUP, rope_dim, seq), jnp.bfloat16),
            pltpu.VMEM((rows, heads, latent_dim), jnp.bfloat16),
            pltpu.VMEM(w_uv.shape, jnp.bfloat16),
            dma((BUFFERS, GROUP)), dma((BUFFERS, GROUP)), dma(()), dma((2,)),
        ],
        compiler_params=pltpu.CompilerParams(vmem_limit_bytes=60 * 1000 * 1000),
        name='attend',
    )(cache_len, q_abs, q_pe, ckv_new, kpe_new, ckv_cache, jnp.swapaxes(kpe_cache, 1, 2), w_uv)


DQ_W = 256


def _sides():
    rep = lax.axis_index('rep')
    me = lax.axis_index('dp')
    chip = me // 2
    core = lax.rem(me, 2)
    return rep, me, chip, core


def front_kernel(x_ref, gain_ref, gain_q_ref, gain_kv_ref, cos_ref, sin_ref, wdq_ref, wdkv_ref, wuq_ref, wuk_ref,
                 abs_ref, pe_ref, ckv_ref, kpe_ref,
                 dq_buf, dkv_buf, uq_buf, uk_buf, x_recv, cs_recv, a_chip, cq_raw, cq_chip, kv_part, kv_recv, abs_part, pe_part, stat,
                 dq_sem, dkv_sem, uq_sem, uk_sem, in_send, in_recv, cq_send, cq_recv, kv_send, kv_got, abs_send, abs_recv, pe_send, pe_recv, keep_sem):
    rep, me, chip, core = _sides()
    part = chip * 2 + (1 - core)
    rows, d_model = x_ref.shape
    latent_dim = ckv_ref.shape[1]
    rope_dim = kpe_ref.shape[1]
    half_dim = rope_dim // 2
    nope_dim = wuk_ref.shape[2]
    head_dim = nope_dim + rope_dim
    half_k = d_model // 2
    n_dq = dq_buf.shape[0]
    n_uq = uq_buf.shape[0]
    q_rank = cq_chip.shape[1]
    block_rows = HEAD_BLOCK * head_dim
    my_heads = n_uq * HEAD_BLOCK

    def dq_copy(index):
        cols = pl.ds(pl.multiple_of((core * n_dq + index) * DQ_W, DQ_W), DQ_W)
        return pltpu.make_async_copy(wdq_ref.at[:, cols], dq_buf.at[index], dq_sem.at[index])

    def uq_copy(index):
        sel = pl.ds(pl.multiple_of((core * n_uq + index) * block_rows, block_rows), block_rows)
        return pltpu.make_async_copy(wuq_ref.at[sel, :], uq_buf.at[index], uq_sem.at[index])

    my_k = pl.ds(pl.multiple_of(core * half_k, half_k), half_k)
    dkv_copy = pltpu.make_async_copy(wdkv_ref.at[:, my_k], dkv_buf, dkv_sem)
    heads_here = pl.ds(pl.multiple_of(core * my_heads, my_heads), my_heads)
    uk_copy = pltpu.make_async_copy(wuk_ref.at[:, heads_here, :], uk_buf, uk_sem)
    for index in range(n_dq):
        dq_copy(index).start()
    dkv_copy.start()
    uk_copy.start()
    for index in range(n_uq):
        uq_copy(index).start()

    barrier = pltpu.get_barrier_semaphore()
    pl.semaphore_signal(barrier, inc=1, device_id=(rep, part), device_id_type=MESH)
    pl.semaphore_wait(barrier, 1)

    def remote(src, dst, send, recv):
        return pltpu.make_async_remote_copy(src_ref=src, dst_ref=dst, send_sem=send, recv_sem=recv,
                                            device_id=(rep, part), device_id_type=MESH)

    swaps = [remote(x_ref, x_recv, in_send.at[0], in_recv.at[0]),
             remote(cos_ref, cs_recv.at[0], in_send.at[1], in_recv.at[1]),
             remote(sin_ref, cs_recv.at[1], in_send.at[2], in_recv.at[2])]
    for swap in swaps:
        swap.start()

    own = pl.ds(pl.multiple_of(core * rows, rows), rows)
    other = pl.ds(pl.multiple_of((1 - core) * rows, rows), rows)
    n_cols = d_model // OUT_W

    def normalise(src_ref, dst_rows):
        def square_step(index, total_sq):
            vals = src_ref[:, pl.ds(pl.multiple_of(index * OUT_W, OUT_W), OUT_W)].astype(jnp.float32)
            return total_sq + jnp.sum(vals * vals, axis=-1, keepdims=True)

        total_sq = lax.fori_loop(0, n_cols, square_step, jnp.zeros((rows, 1), jnp.float32))
        stat[...] = lax.rsqrt(total_sq * (1.0 / d_model) + EPSILON)

        def scale_step(index, carry):
            cols = pl.ds(pl.multiple_of(index * OUT_W, OUT_W), OUT_W)
            vals = src_ref[:, cols].astype(jnp.float32) * stat[...] * gain_ref[0:1, cols]
            a_chip[dst_rows, cols] = vals.astype(jnp.bfloat16)
            return carry

        lax.fori_loop(0, n_cols, scale_step, 0)

    normalise(x_ref, own)
    for swap in swaps:
        swap.wait()
    normalise(x_recv, other)

    def cq_copy(index):
        blk = cq_raw.at[core * n_dq + index]
        return remote(blk, blk, cq_send.at[index], cq_recv.at[index])

    def dq_step(index, carry):
        dq_copy(index).wait()
        cq_raw[core * n_dq + index] = jnp.dot(a_chip[...], dq_buf[index], preferred_element_type=jnp.float32)
        cq_copy(index).start()
        return carry

    lax.fori_loop(0, n_dq, dq_step, 0)

    dkv_copy.wait()
    kv_part[...] = lax.dot_general(a_chip[:, my_k], dkv_buf[...], NT, preferred_element_type=jnp.float32)
    kv_copy = remote(kv_part.at[other, :], kv_recv, kv_send, kv_got)
    kv_copy.start()

    for index in range(n_dq):
        cq_copy(index).wait()
    total_sq = jnp.zeros((2 * rows, 1), jnp.float32)
    for index in range(2 * n_dq):
        vals = cq_raw[index]
        total_sq += jnp.sum(vals * vals, axis=-1, keepdims=True)
    inv = lax.rsqrt(total_sq * (1.0 / q_rank) + EPSILON)
    for index in range(2 * n_dq):
        for lane in range(0, DQ_W, 128):
            start = index * DQ_W + lane
            gain = gain_q_ref[start // 128:start // 128 + 1, :]
            cq_chip[:, start:start + 128] = (cq_raw[index, :, lane:lane + 128] * inv * gain).astype(jnp.bfloat16)

    cos_own, sin_own = cos_ref[...].T, sin_ref[...].T
    cos_far, sin_far = cs_recv[0].T, cs_recv[1].T
    first = core == 0
    cos_t = jnp.concatenate([jnp.where(first, cos_own, cos_far), jnp.where(first, cos_far, cos_own)], axis=0)
    sin_t = jnp.concatenate([jnp.where(first, sin_own, sin_far), jnp.where(first, sin_far, sin_own)], axis=0)
    uk_copy.wait()

    def head_cols(index):
        return pl.ds(pl.multiple_of(core * my_heads + index * SWAP_BLOCK, SWAP_BLOCK), SWAP_BLOCK)

    def abs_copy(index):
        return remote(abs_part.at[index, other], abs_ref.at[:, head_cols(index), :], abs_send.at[index], abs_recv.at[index])

    def pe_copy(index):
        return remote(pe_part.at[index, other], pe_ref.at[:, head_cols(index), :], pe_send.at[index], pe_recv.at[index])

    def abs_keep(index):
        return pltpu.make_async_copy(abs_part.at[index, own], abs_ref.at[:, head_cols(index), :], keep_sem.at[0, index])

    def pe_keep(index):
        return pltpu.make_async_copy(pe_part.at[index, own], pe_ref.at[:, head_cols(index), :], keep_sem.at[1, index])

    per_swap = SWAP_BLOCK // HEAD_BLOCK

    def uq_step(index, carry):
        absorbed = []
        turned = []
        for sub in range(per_swap):
            uq_copy(index * per_swap + sub).wait()
        wuk = jnp.swapaxes(uk_buf[:, pl.ds(pl.multiple_of(index * SWAP_BLOCK, SWAP_BLOCK), SWAP_BLOCK), :], 0, 1)
        for sub in range(per_swap):
            q_val = lax.dot_general(cq_chip[...], uq_buf[index * per_swap + sub], NT, preferred_element_type=jnp.float32)
            for head in range(HEAD_BLOCK):
                base = head * head_dim
                nope = q_val[:, base:base + nope_dim].astype(jnp.bfloat16)
                low_half = q_val[:, base + nope_dim:base + nope_dim + half_dim]
                high_half = q_val[:, base + nope_dim + half_dim:base + head_dim]
                turned.append(jnp.concatenate([low_half * cos_t - high_half * sin_t, high_half * cos_t + low_half * sin_t], axis=1).astype(jnp.bfloat16))
                absorbed.append(lax.dot_general(nope, wuk[sub * HEAD_BLOCK + head], NT, preferred_element_type=jnp.float32).astype(jnp.bfloat16))
        abs_part[index] = jnp.swapaxes(jnp.stack(absorbed, axis=0), 0, 1)
        pe_part[index] = jnp.swapaxes(jnp.stack(turned, axis=0), 0, 1)
        for move in (abs_copy, pe_copy, abs_keep, pe_keep):
            move(index).start()
        return carry

    n_swap = n_uq // per_swap
    lax.fori_loop(0, n_swap, uq_step, 0)

    kv_copy.wait()
    kv_val = kv_part[own, :] + kv_recv[...]
    latent = kv_val[:, :latent_dim]
    inv = lax.rsqrt(jnp.mean(latent * latent, axis=-1, keepdims=True) + EPSILON)
    ckv_ref[...] = (latent * inv * gain_kv_ref[...]).astype(jnp.bfloat16)
    low_half = kv_val[:, latent_dim:latent_dim + half_dim]
    high_half = kv_val[:, latent_dim + half_dim:]
    kpe_ref[...] = jnp.concatenate([low_half * cos_own - high_half * sin_own, high_half * cos_own + low_half * sin_own], axis=1).astype(jnp.bfloat16)
    for index in range(n_swap):
        for move in (abs_copy, pe_copy, abs_keep, pe_keep):
            move(index).wait()


def front(hidden, norm_attn, w_dq, norm_q, w_uq, w_dkv, norm_kv, w_uk, rope_cos, rope_sin):
    rows, d_model = hidden.shape
    latent_dim, heads, nope_dim = w_uk.shape
    q_rank, _, head_dim = w_uq.shape
    rope_dim = head_dim - nope_dim
    half_dim = rope_dim // 2
    kv_dim = w_dkv.shape[1]
    n_dq = q_rank // 2 // DQ_W
    n_uq = heads // 2 // HEAD_BLOCK
    n_swap = heads // 2 // SWAP_BLOCK
    f32, bf16 = jnp.float32, jnp.bfloat16
    vmem = pl.BlockSpec(memory_space=pltpu.VMEM)
    anywhere = pl.BlockSpec(memory_space=pl.ANY)
    dma = pltpu.SemaphoreType.DMA
    return pl.pallas_call(
        front_kernel,
        out_shape=[
            jax.ShapeDtypeStruct((rows, heads, latent_dim), bf16),
            jax.ShapeDtypeStruct((rows, heads, rope_dim), bf16),
            jax.ShapeDtypeStruct((rows, latent_dim), bf16),
            jax.ShapeDtypeStruct((rows, rope_dim), bf16),
        ],
        in_specs=[vmem] * 6 + [anywhere] * 4,
        out_specs=[anywhere, anywhere, vmem, vmem],
        scratch_shapes=[
            pltpu.VMEM((n_dq, d_model, DQ_W), bf16),
            pltpu.VMEM((kv_dim, d_model // 2), bf16),
            pltpu.VMEM((n_uq, HEAD_BLOCK * head_dim, q_rank), bf16),
            pltpu.VMEM((latent_dim, heads // 2, nope_dim), bf16),
            pltpu.VMEM((rows, d_model), bf16),
            pltpu.VMEM((2, half_dim, rows), f32),
            pltpu.VMEM((2 * rows, d_model), bf16),
            pltpu.VMEM((2 * n_dq, 2 * rows, DQ_W), f32),
            pltpu.VMEM((2 * rows, q_rank), bf16),
            pltpu.VMEM((2 * rows, kv_dim), f32),
            pltpu.VMEM((rows, kv_dim), f32),
            pltpu.VMEM((n_swap, 2 * rows, SWAP_BLOCK, latent_dim), bf16),
            pltpu.VMEM((n_swap, 2 * rows, SWAP_BLOCK, rope_dim), bf16),
            pltpu.VMEM((rows, 1), f32),
            dma((n_dq,)), dma(()), dma((n_uq,)), dma(()), dma((3,)), dma((3,)), dma((n_dq,)), dma((n_dq,)), dma(()), dma(()),
            dma((n_swap,)), dma((n_swap,)), dma((n_swap,)), dma((n_swap,)), dma((2, n_swap)),
        ],
        compiler_params=pltpu.CompilerParams(collective_id=1, has_side_effects=True, vmem_limit_bytes=66 * 1000 * 1000),
        name='front',
    )(hidden, norm_attn.reshape(1, -1), norm_q.reshape(-1, 128), norm_kv.reshape(1, -1), rope_cos.T, rope_sin.T,
      w_dq, w_dkv.T, jnp.transpose(w_uq, (1, 2, 0)).reshape(heads * head_dim, q_rank), w_uk)


def attention_rows(hidden, ckv_cache, kpe_cache, cache_len, rope_cos, rope_sin, norm_attn, w_dq, norm_q, w_uq, w_dkv, norm_kv, w_uk, w_uv):
    score_scale = MSCALE * MSCALE / math.sqrt(w_uq.shape[2])
    q_abs, q_pe, ckv_new, kpe_new = front(hidden, norm_attn, w_dq, norm_q, w_uq, w_dkv, norm_kv, w_uk, rope_cos, rope_sin)
    head_out, ckv_new, kpe_new = attend(q_abs, q_pe, ckv_new, kpe_new, ckv_cache, kpe_cache, cache_len, w_uv, score_scale)
    return head_out, ckv_new, kpe_new


def tail_kernel(o_ref, x_ref, gain_ref, wout_ref, wgate_ref, wup_ref, wdown_ref, out_ref,
                slots, o_chip, x_chip, x_own, r_all, u_all, gate_buf, up_buf, act, sq_acc, pair_send, pair_recv, far_send, far_recv, own_sum,
                slot_sem, in_send, in_recv, loc_sem, rp_send, rp_recv, rx_send, rx_recv, rf_send, rf_recv,
                pp_send, pp_recv, px_send, px_recv):
    rep, me, chip, core = _sides()
    part = chip * 2 + (1 - core)
    opp = (1 - chip) * 2 + core
    diag = (1 - chip) * 2 + (1 - core)
    attn_k = wout_ref.shape[0]
    d_model = wgate_ref.shape[0]
    ff = wgate_ref.shape[1]
    rows = x_ref.shape[0]
    half = d_model // 2
    n_out = half // OUT_W
    n_ff = ff // OUT_W
    n_down = d_model // OUT_W
    first_ff = n_out
    first_down = n_out + 2 * n_ff
    total = first_down + n_down
    pieces = OUT_W // PIECE
    n_half = half // PIECE
    n_all = d_model // PIECE

    def col(index):
        return pl.ds(pl.multiple_of(index * OUT_W, OUT_W), OUT_W)

    def piece(index):
        return pl.ds(pl.multiple_of(index * PIECE, PIECE), PIECE)

    def row_block(owner, count=1):
        return pl.ds(pl.multiple_of(owner * rows, rows), count * rows)

    def slot_copy(kind, index, step):
        slot = lax.rem(step, SLOTS)
        src = {'out': wout_ref, 'gate': wgate_ref, 'up': wup_ref, 'down': wdown_ref}[kind]
        depth = src.shape[0]
        return pltpu.make_async_copy(src.at[:, col(index)], slots.at[slot, pl.ds(0, depth), :], slot_sem.at[slot])

    def fetch(step):
        @pl.when(step < first_ff)
        def _():
            slot_copy('out', core * n_out + step, step).start()

        @pl.when((step >= first_ff) & (step < first_down) & (lax.rem(step - first_ff, 2) == 0))
        def _():
            slot_copy('gate', (step - first_ff) // 2, step).start()

        @pl.when((step >= first_ff) & (step < first_down) & (lax.rem(step - first_ff, 2) == 1))
        def _():
            slot_copy('up', (step - first_ff) // 2, step).start()

        @pl.when((step >= first_down) & (step < total))
        def _():
            slot_copy('down', step - first_down, step).start()

    my_rows = row_block(core)
    my_half = pl.ds(pl.multiple_of(core * half, half), half)
    their_half = pl.ds(pl.multiple_of((1 - core) * half, half), half)
    keep_o = pltpu.make_async_copy(o_ref, o_chip.at[my_rows, :], loc_sem.at[0])
    keep_x = pltpu.make_async_copy(x_ref.at[:, my_half], x_chip.at[my_rows, :], loc_sem.at[1])
    give_x = pltpu.make_async_copy(x_ref.at[:, their_half], x_own, loc_sem.at[2])
    keep_o.start()
    give_x.start()
    keep_x.start()
    slot_copy('out', core * n_out, 0).start()

    barrier = pltpu.get_barrier_semaphore()
    for peer in (part, opp):
        pl.semaphore_signal(barrier, inc=1, device_id=(rep, peer), device_id_type=MESH)
    pl.semaphore_wait(barrier, 2)

    def remote(src, dst, send, recv, peer):
        return pltpu.make_async_remote_copy(src_ref=src, dst_ref=dst, send_sem=send, recv_sem=recv,
                                            device_id=(rep, peer), device_id_type=MESH)

    keep_o.wait()
    send_o = remote(o_chip.at[my_rows, :], o_chip.at[my_rows, :], in_send.at[0], in_recv.at[0], part)
    send_o.start()
    give_x.wait()
    send_x = remote(x_own, x_chip.at[my_rows, :], in_send.at[1], in_recv.at[1], part)
    send_x.start()
    for step in range(1, SLOTS):
        slot_copy('out', core * n_out + step, step).start()
    sq_acc[...] = jnp.zeros_like(sq_acc)
    gate_buf[...] = jnp.zeros_like(gate_buf)
    up_buf[...] = jnp.zeros_like(up_buf)
    keep_x.wait()
    send_o.wait()
    send_x.wait()

    chip_rows = row_block(chip * 2, 2)
    far_rows = row_block((1 - chip) * 2, 2)

    def r_pair(index):
        blk = r_all.at[core * n_half + index, chip_rows, :]
        return remote(blk, blk, rp_send.at[index], rp_recv.at[index], part)

    def r_far(index):
        blk = r_all.at[core * n_half + index, chip_rows, :]
        return remote(blk, blk, rx_send.at[index], rx_recv.at[index], opp)

    def r_forward(index):
        blk = r_all.at[core * n_half + index, far_rows, :]
        return remote(blk, blk, rf_send.at[index], rf_recv.at[index], part)

    def add_squares(sel, vals):
        wide = vals.astype(jnp.float32)
        wide = wide * wide
        acc = sq_acc[sel, :]
        for lane in range(0, PIECE, 128):
            acc = acc + wide[:, lane:lane + 128]
        sq_acc[sel, :] = acc

    def take_pair(index):
        r_pair(index).wait_recv()
        add_squares(chip_rows, r_all[(1 - core) * n_half + index, chip_rows, :])

    def take_far(index):
        r_far(index).wait_recv()
        r_forward(index).start()
        add_squares(far_rows, r_all[core * n_half + index, far_rows, :])

    def take_forward(index):
        r_forward(index).wait_recv()
        add_squares(far_rows, r_all[(1 - core) * n_half + index, far_rows, :])

    lags = ((take_pair, 2), (take_far, 4), (take_forward, 6))

    def out_step(index, carry):
        slot_copy('out', core * n_out + index, index).wait()
        for sub in range(pieces):
            here = index * pieces + sub
            acc = jnp.dot(o_chip[...], slots[lax.rem(index, SLOTS), :attn_k, sub * PIECE:(sub + 1) * PIECE], preferred_element_type=jnp.float32)
            vals = (x_chip[:, piece(here)].astype(jnp.float32) + acc).astype(jnp.bfloat16)
            r_all[core * n_half + here, chip_rows, :] = vals
            r_far(here).start()
            r_pair(here).start()
            add_squares(chip_rows, vals)
            for take, lag in lags:
                @pl.when(here >= lag)
                def _(take=take, lag=lag):
                    take(here - lag)
        fetch(index + SLOTS)
        return carry

    lax.fori_loop(0, n_out, out_step, 0)

    def inverse(owner):
        total_sq = jnp.sum(sq_acc[row_block(owner), :], axis=-1, keepdims=True)
        return lax.rsqrt(total_sq * (1.0 / d_model) + EPSILON)

    def normalise(places):
        invs = [inverse(owner) for _, owner in places]

        def norm_step(index, carry):
            for (place, owner), inv in zip(places, carry):
                vals = r_all[index, row_block(owner), :].astype(jnp.float32) * inv * gain_ref[0:1, piece(index)]
                u_all[place * rows:(place + 1) * rows, piece(index)] = vals.astype(jnp.bfloat16)
            return carry

        lax.fori_loop(0, n_all, norm_step, tuple(invs))

    for index in range(n_half - 2, n_half):
        take_pair(index)
    take_far(n_half - 4)
    take_forward(n_half - 6)
    take_far(n_half - 3)
    take_forward(n_half - 5)
    normalise(((0, part), (1, me)))
    near = slice(0, 2 * rows)
    far = slice(2 * rows, 4 * rows)

    def activate(gate_val, up_val):
        return (gate_val * jax.nn.sigmoid(gate_val) * up_val).astype(jnp.bfloat16)

    def product(sel, step):
        return jnp.dot(u_all[sel, :], slots[lax.rem(step, SLOTS), :d_model, :], preferred_element_type=jnp.float32)

    def early(index, sel):
        step = first_ff + 2 * index
        gate_val = product(sel, step)
        act[sel, index * OUT_W:(index + 1) * OUT_W] = activate(gate_val, product(sel, step + 1))

    for index in range(EARLY):
        slot_copy('gate', index, first_ff + 2 * index).wait()
        slot_copy('up', index, first_ff + 2 * index + 1).wait()
        early(index, near)
        if index == 0:
            take_far(n_half - 2)
            take_far(n_half - 1)
            take_forward(n_half - 4)
            take_forward(n_half - 3)
    take_forward(n_half - 2)
    take_forward(n_half - 1)
    normalise(((2, diag), (3, opp)))
    for index in range(EARLY):
        early(index, far)
        fetch(first_ff + 2 * index + SLOTS)
        fetch(first_ff + 2 * index + 1 + SLOTS)

    def ff_step(index, carry):
        step = first_ff + 2 * index
        now, before = lax.rem(index, 2), lax.rem(index + 1, 2)
        slot_copy('gate', index, step).wait()
        act[:, col(jnp.maximum(index - 1, EARLY))] = activate(gate_buf[before], up_buf[...])
        gate_buf[now] = product(slice(None), step)
        fetch(step + SLOTS)
        slot_copy('up', index, step + 1).wait()
        up_buf[...] = product(slice(None), step + 1)
        fetch(step + 1 + SLOTS)
        return carry

    lax.fori_loop(EARLY, n_ff, ff_step, 0)
    act[:, (n_ff - 1) * OUT_W:] = activate(gate_buf[(n_ff - 1) % 2], up_buf[...])

    def pair_copy(index):
        return remote(pair_send.at[index], pair_recv.at[index], pp_send.at[index], pp_recv.at[index], part)

    def far_copy(index):
        return remote(far_send.at[index], far_recv.at[index], px_send.at[index], px_recv.at[index], opp)

    def combine(index):
        pair_copy(index).wait_recv()
        far_send[index] += pair_recv[index, rows:, :]
        far_copy(index).start()
        own_sum[index] += pair_recv[index, :rows, :]

    def down_step(index, carry):
        step = first_down + index
        slot_copy('down', index, step).wait()
        for sub in range(pieces):
            here = index * pieces + sub
            part_sum = jnp.dot(act[...], slots[lax.rem(step, SLOTS), :ff, sub * PIECE:(sub + 1) * PIECE], preferred_element_type=jnp.float32)
            pair_send[here, :rows] = part_sum[:rows]
            pair_send[here, rows:] = part_sum[2 * rows:3 * rows]
            own_sum[here] = part_sum[rows:2 * rows]
            far_send[here] = part_sum[3 * rows:]
            pair_copy(here).start()

            @pl.when(here >= 1)
            def _():
                combine(here - 1)
        fetch(step + SLOTS)
        return carry

    lax.fori_loop(0, n_down, down_step, 0)
    combine(n_all - 1)

    def settle(index, carry):
        r_pair(index).wait_send()
        r_far(index).wait_send()
        r_forward(index).wait_send()
        return carry

    lax.fori_loop(0, n_half, settle, 0)
    own_rows = row_block(me)

    def finish(index, carry):
        far_copy(index).wait()
        pair_copy(index).wait_send()
        mlp = own_sum[index] + far_recv[index]
        out_ref[:, piece(index)] = (r_all[index, own_rows, :].astype(jnp.float32) + mlp).astype(jnp.bfloat16)
        return carry

    lax.fori_loop(0, n_all, finish, 0)


def tail(head_out, hidden, norm_mlp, w_out, w_gate, w_up, w_down):
    rows, d_model = hidden.shape
    attn_k = w_out.shape[0]
    ff = w_gate.shape[1]
    n_half = d_model // 2 // PIECE
    n_all = d_model // PIECE
    depth = max(attn_k, d_model, ff)
    vmem = pl.BlockSpec(memory_space=pltpu.VMEM)
    anywhere = pl.BlockSpec(memory_space=pl.ANY)
    dma = pltpu.SemaphoreType.DMA
    f32, bf16 = jnp.float32, jnp.bfloat16
    return pl.pallas_call(
        tail_kernel,
        out_shape=jax.ShapeDtypeStruct((rows, d_model), bf16),
        in_specs=[anywhere, anywhere, vmem, anywhere, anywhere, anywhere, anywhere],
        out_specs=vmem,
        scratch_shapes=[
            pltpu.VMEM((SLOTS, depth, OUT_W), bf16),
            pltpu.VMEM((2 * rows, attn_k), bf16),
            pltpu.VMEM((2 * rows, d_model // 2), bf16),
            pltpu.VMEM((rows, d_model // 2), bf16),
            pltpu.VMEM((n_all, 4 * rows, PIECE), bf16),
            pltpu.VMEM((4 * rows, d_model), bf16),
            pltpu.VMEM((2, 4 * rows, OUT_W), f32),
            pltpu.VMEM((4 * rows, OUT_W), f32),
            pltpu.VMEM((4 * rows, ff), bf16),
            pltpu.VMEM((4 * rows, 128), f32),
            pltpu.VMEM((n_all, 2 * rows, PIECE), f32),
            pltpu.VMEM((n_all, 2 * rows, PIECE), f32),
            pltpu.VMEM((n_all, rows, PIECE), f32),
            pltpu.VMEM((n_all, rows, PIECE), f32),
            pltpu.VMEM((n_all, rows, PIECE), f32),
            dma((SLOTS,)), dma((2,)), dma((2,)), dma((3,)),
            dma((n_half,)), dma((n_half,)), dma((n_half,)), dma((n_half,)), dma((n_half,)), dma((n_half,)),
            dma((n_all,)), dma((n_all,)), dma((n_all,)), dma((n_all,)),
        ],
        compiler_params=pltpu.CompilerParams(collective_id=0, has_side_effects=True, vmem_limit_bytes=66 * 1000 * 1000),
        name='tail',
    )(head_out, hidden, norm_mlp.reshape(1, d_model), w_out, w_gate, w_up, w_down)


def solution(mesh):
    row_spec = P(('rep', 'dp'), None)
    cube_spec = P(('rep', 'dp'), None, None)
    full_spec = P()
    in_specs = (row_spec, cube_spec, cube_spec, P(('rep', 'dp')), row_spec, row_spec,
                full_spec, full_spec, full_spec, full_spec, full_spec, full_spec, full_spec, full_spec, full_spec, full_spec,
                P(None, 'dp'), P(None, 'dp'), P('dp', None))

    def local_step(hidden, ckv_cache, kpe_cache, cache_len, rope_cos, rope_sin, norm_attn, w_dq, norm_q, w_uq, w_dkv, norm_kv, w_uk, w_uv, w_out, norm_mlp, w_gate, w_up, w_down):
        head_out, ckv_new, kpe_new = attention_rows(hidden, ckv_cache, kpe_cache, cache_len, rope_cos, rope_sin, norm_attn, w_dq, norm_q, w_uq, w_dkv, norm_kv, w_uk, w_uv)
        out_hidden = tail(head_out, hidden, norm_mlp, w_out.reshape(-1, w_out.shape[-1]), w_gate, w_up, w_down)
        return out_hidden, ckv_new, kpe_new

    return jax.shard_map(local_step, mesh=mesh, in_specs=in_specs, out_specs=(row_spec, row_spec, row_spec), check_vma=False)
```

```python
import functools
import math
import jax
import jax.numpy as jnp
from jax import lax
from jax.experimental import pallas as pl
from jax.experimental.pallas import tpu as pltpu
from jax.sharding import PartitionSpec as P

EPSILON = 1e-6
MSCALE = 0.1 * math.log(40.0) + 1.0
MESH = pl.DeviceIdType.MESH


OUT_W = 512
PIECE = 256
SLOTS = 4
EARLY = 2
HEAD_BLOCK = 8
SWAP_BLOCK = 16
NT = (((1,), (1,)), ((), ()))
NN = (((1,), (0,)), ((), ()))


GROUP = 8
BUFFERS = 3
CHUNK = 128


def attend_kernel(score_scale, len_ref, abs_hbm, pe_hbm, new_ref, pe_new_ref, ckv_ref, kpe_ref, wuv_ref,
                  out_ref, new_out_ref, pe_out_ref, order_buf, turned_buf, abs_ref, pe_ref, kv_buf, kp_buf, lat_buf, wuv_buf, kv_sem, kp_sem, wuv_sem, query_sem):
    query_copies = [pltpu.make_async_copy(abs_hbm, abs_ref, query_sem.at[0]), pltpu.make_async_copy(pe_hbm, pe_ref, query_sem.at[1])]
    for made in query_copies:
        made.start()
    rows, heads, latent_dim = abs_ref.shape
    seq = ckv_ref.shape[1]
    variants = seq // CHUNK
    groups = rows // GROUP
    value_dim = wuv_ref.shape[2]

    def chunks_of(row):
        return len_ref[row] // CHUNK

    def count_step(row, tally):
        return tuple(count + (chunks_of(row) == which).astype(jnp.int32) for which, count in enumerate(tally))

    tally = lax.fori_loop(0, rows, count_step, (jnp.int32(0),) * variants)
    starts = [jnp.int32(0)]
    for which in range(variants - 1):
        starts.append(starts[-1] + tally[which])

    def place_step(row, heads_of):
        mine = [chunks_of(row) == which for which in range(variants)]
        place = sum(jnp.where(hit, head, 0) for hit, head in zip(mine, heads_of))
        order_buf[place] = row
        return tuple(head + hit.astype(jnp.int32) for hit, head in zip(mine, heads_of))

    lax.fori_loop(0, rows, place_step, tuple(starts))

    def group_chunks(group):
        return chunks_of(order_buf[group * GROUP + GROUP - 1]) + 1

    def copies(group, size):
        slot = lax.rem(group, BUFFERS)
        made = []
        for place in range(GROUP):
            row = order_buf[group * GROUP + place]
            made.append(pltpu.make_async_copy(ckv_ref.at[row, pl.ds(0, size), :], kv_buf.at[slot, place, pl.ds(0, size), :], kv_sem.at[slot, place]))
            made.append(pltpu.make_async_copy(kpe_ref.at[row, :, pl.ds(0, size)], kp_buf.at[slot, place, :, pl.ds(0, size)], kp_sem.at[slot, place]))
        return made

    def start(group):
        for count in range(1, variants + 1):
            @pl.when(group_chunks(group) == count)
            def _():
                for made in copies(group, count * CHUNK):
                    made.start()

    for group in range(BUFFERS - 1):
        start(group)
    wuv_copy = pltpu.make_async_copy(wuv_ref, wuv_buf, wuv_sem)
    turned_buf[...] = pe_new_ref[...].astype(jnp.float32).T
    new_out_ref[...] = new_ref[...]
    pe_out_ref[...] = pe_new_ref[...]

    def compute(group, size):
        slot = lax.rem(group, BUFFERS)
        for made in copies(group, size):
            made.wait()
        rows_of = [order_buf[group * GROUP + place] for place in range(GROUP)]
        for place, row in enumerate(rows_of):
            length = len_ref[row]
            base = pl.multiple_of((row // 16) * 16, 16)
            picked = new_ref[pl.ds(base, 16), :].astype(jnp.float32)
            hit = lax.broadcasted_iota(jnp.int32, picked.shape, 0) == row - base
            new = jnp.sum(jnp.where(hit, picked, 0.0), axis=0, keepdims=True)
            hit = lax.broadcasted_iota(jnp.int32, turned_buf.shape, 1) == row
            new_pe = jnp.sum(jnp.where(hit, turned_buf[...], 0.0), axis=1, keepdims=True)
            base = pl.multiple_of((length // 16) * 16, 16)
            block = kv_buf[slot, place, pl.ds(base, 16), :]
            hit = lax.broadcasted_iota(jnp.int32, block.shape, 0) == length - base
            kv_buf[slot, place, pl.ds(base, 16), :] = jnp.where(hit, new, block.astype(jnp.float32)).astype(jnp.bfloat16)
            lane = pl.multiple_of((length // CHUNK) * CHUNK, CHUNK)
            block = kp_buf[slot, place, :, pl.ds(lane, CHUNK)]
            hit = lax.broadcasted_iota(jnp.int32, block.shape, 1) == length - lane
            kp_buf[slot, place, :, pl.ds(lane, CHUNK)] = jnp.where(hit, new_pe, block.astype(jnp.float32)).astype(jnp.bfloat16)
        all_scores = [(lax.dot_general(abs_ref[row], kv_buf[slot, place, :size, :], NT, preferred_element_type=jnp.float32)
                       + jnp.dot(pe_ref[row], kp_buf[slot, place, :, :size], preferred_element_type=jnp.float32)) * score_scale
                      for place, row in enumerate(rows_of)]
        weights = []
        for place, row in enumerate(rows_of):
            positions = lax.broadcasted_iota(jnp.int32, (heads, size), 1)
            scores = jnp.where(positions <= len_ref[row], all_scores[place], -jnp.inf)
            exp_all = jnp.exp(scores - jnp.max(scores, axis=1, keepdims=True))
            weights.append((exp_all.astype(jnp.bfloat16), jnp.sum(exp_all, axis=1, keepdims=True)))
        for place, row in enumerate(rows_of):
            weighted = jnp.dot(weights[place][0], kv_buf[slot, place, :size, :], preferred_element_type=jnp.float32)
            lat_buf[row] = (weighted / weights[place][1]).astype(jnp.bfloat16)

    def group_step(group, carry):
        @pl.when(group == groups - 3)
        def _():
            wuv_copy.start()

        @pl.when(group + BUFFERS - 1 < groups)
        def _():
            start(group + BUFFERS - 1)
        for count in range(1, variants + 1):
            @pl.when(group_chunks(group) == count)
            def _():
                compute(group, count * CHUNK)
        return carry

    for made in query_copies:
        made.wait()
    lax.fori_loop(0, groups, group_step, 0)
    wuv_copy.wait()

    def value_step(block, carry):
        sel = pl.ds(pl.multiple_of(block * SWAP_BLOCK, SWAP_BLOCK), SWAP_BLOCK)
        lat = jnp.swapaxes(lat_buf[:, sel, :], 0, 1)
        wuv = jnp.swapaxes(wuv_buf[:, sel, :], 0, 1)
        for head in range(SWAP_BLOCK):
            dst = pl.ds(pl.multiple_of(block * SWAP_BLOCK * value_dim + head * value_dim, value_dim), value_dim)
            out_ref[:, dst] = jnp.dot(lat[head], wuv[head], preferred_element_type=jnp.float32).astype(jnp.bfloat16)
        return carry

    lax.fori_loop(0, heads // SWAP_BLOCK, value_step, 0)


def attend(q_abs, q_pe, ckv_new, kpe_new, ckv_cache, kpe_cache, cache_len, w_uv, score_scale):
    rows, heads, latent_dim = q_abs.shape
    rope_dim = q_pe.shape[2]
    seq = ckv_cache.shape[1]
    value_dim = w_uv.shape[2]
    smem = pl.BlockSpec(memory_space=pltpu.SMEM)
    vmem = pl.BlockSpec(memory_space=pltpu.VMEM)
    anywhere = pl.BlockSpec(memory_space=pl.ANY)
    dma = pltpu.SemaphoreType.DMA
    return pl.pallas_call(
        functools.partial(attend_kernel, score_scale),
        out_shape=[jax.ShapeDtypeStruct((rows, heads * value_dim), jnp.bfloat16),
                   jax.ShapeDtypeStruct(ckv_new.shape, jnp.bfloat16), jax.ShapeDtypeStruct(kpe_new.shape, jnp.bfloat16)],
        in_specs=[smem, anywhere, anywhere, vmem, vmem, anywhere, anywhere, anywhere],
        out_specs=[vmem, vmem, vmem],
        scratch_shapes=[
            pltpu.SMEM((rows,), jnp.int32),
            pltpu.VMEM((rope_dim, rows), jnp.float32),
            pltpu.VMEM(q_abs.shape, jnp.bfloat16),
            pltpu.VMEM(q_pe.shape, jnp.bfloat16),
            pltpu.VMEM((BUFFERS, GROUP, seq, latent_dim), jnp.bfloat16),
            pltpu.VMEM((BUFFERS, GROUP, rope_dim, seq), jnp.bfloat16),
            pltpu.VMEM((rows, heads, latent_dim), jnp.bfloat16),
            pltpu.VMEM(w_uv.shape, jnp.bfloat16),
            dma((BUFFERS, GROUP)), dma((BUFFERS, GROUP)), dma(()), dma((2,)),
        ],
        compiler_params=pltpu.CompilerParams(vmem_limit_bytes=60 * 1000 * 1000),
        name='attend',
    )(cache_len, q_abs, q_pe, ckv_new, kpe_new, ckv_cache, jnp.swapaxes(kpe_cache, 1, 2), w_uv)


DQ_W = 256


def _sides():
    rep = lax.axis_index('rep')
    me = lax.axis_index('dp')
    chip = me // 2
    core = lax.rem(me, 2)
    return rep, me, chip, core


def front_kernel(x_ref, gain_ref, gain_q_ref, gain_kv_ref, cos_ref, sin_ref, wdq_ref, wdkv_ref, wuq_ref, wuk_ref,
                 abs_ref, pe_ref, ckv_ref, kpe_ref,
                 dq_buf, dkv_buf, uq_buf, uk_buf, wuk_buf, x_own, x_recv, cs_recv, a_chip, cq_raw, cq_chip, kv_part, kv_recv, abs_part, pe_part, stat,
                 x_sem, dq_sem, dkv_sem, uq_sem, uk_sem, in_send, in_recv, cq_send, cq_recv, kv_send, kv_got, abs_send, abs_recv, pe_send, pe_recv, keep_sem):
    rep, me, chip, core = _sides()
    part = chip * 2 + (1 - core)
    rows, d_model = x_ref.shape
    latent_dim = ckv_ref.shape[1]
    rope_dim = kpe_ref.shape[1]
    half_dim = rope_dim // 2
    nope_dim = wuk_ref.shape[2]
    head_dim = nope_dim + rope_dim
    half_k = d_model // 2
    n_dq = dq_buf.shape[0]
    n_uq = uq_buf.shape[0]
    q_rank = cq_chip.shape[1]
    block_rows = HEAD_BLOCK * head_dim
    my_heads = n_uq * HEAD_BLOCK

    def dq_copy(index):
        cols = pl.ds(pl.multiple_of((core * n_dq + index) * DQ_W, DQ_W), DQ_W)
        return pltpu.make_async_copy(wdq_ref.at[:, cols], dq_buf.at[index], dq_sem.at[index])

    def uq_copy(index):
        sel = pl.ds(pl.multiple_of((core * n_uq + index) * block_rows, block_rows), block_rows)
        return pltpu.make_async_copy(wuq_ref.at[sel, :], uq_buf.at[index], uq_sem.at[index])

    my_k = pl.ds(pl.multiple_of(core * half_k, half_k), half_k)
    dkv_copy = pltpu.make_async_copy(wdkv_ref.at[:, my_k], dkv_buf, dkv_sem)
    heads_here = pl.ds(pl.multiple_of(core * my_heads, my_heads), my_heads)
    uk_copy = pltpu.make_async_copy(wuk_ref.at[:, heads_here, :], uk_buf, uk_sem)
    x_copy = pltpu.make_async_copy(x_ref, x_own, x_sem)
    x_copy.start()
    dq_copy(0).start()

    barrier = pltpu.get_barrier_semaphore()
    pl.semaphore_signal(barrier, inc=1, device_id=(rep, part), device_id_type=MESH)
    pl.semaphore_wait(barrier, 1)

    def remote(src, dst, send, recv):
        return pltpu.make_async_remote_copy(src_ref=src, dst_ref=dst, send_sem=send, recv_sem=recv,
                                            device_id=(rep, part), device_id_type=MESH)

    x_copy.wait()
    swaps = [remote(x_own, x_recv, in_send.at[0], in_recv.at[0]),
             remote(cos_ref, cs_recv.at[0], in_send.at[1], in_recv.at[1]),
             remote(sin_ref, cs_recv.at[1], in_send.at[2], in_recv.at[2])]
    for swap in swaps:
        swap.start()
    for index in range(1, n_dq):
        dq_copy(index).start()
    uk_copy.start()
    for index in range(n_uq):
        uq_copy(index).start()
    dkv_copy.start()

    own = pl.ds(pl.multiple_of(core * rows, rows), rows)
    other = pl.ds(pl.multiple_of((1 - core) * rows, rows), rows)
    n_cols = d_model // OUT_W

    def normalise(src_ref, dst_rows):
        def square_step(index, total_sq):
            vals = src_ref[:, pl.ds(pl.multiple_of(index * OUT_W, OUT_W), OUT_W)].astype(jnp.float32)
            return total_sq + jnp.sum(vals * vals, axis=-1, keepdims=True)

        total_sq = lax.fori_loop(0, n_cols, square_step, jnp.zeros((rows, 1), jnp.float32))
        stat[...] = lax.rsqrt(total_sq * (1.0 / d_model) + EPSILON)

        def scale_step(index, carry):
            cols = pl.ds(pl.multiple_of(index * OUT_W, OUT_W), OUT_W)
            vals = src_ref[:, cols].astype(jnp.float32) * stat[...] * gain_ref[0:1, cols]
            a_chip[dst_rows, cols] = vals.astype(jnp.bfloat16)
            return carry

        lax.fori_loop(0, n_cols, scale_step, 0)

    normalise(x_own, own)
    for swap in swaps:
        swap.wait()
    normalise(x_recv, other)

    def cq_copy(index):
        blk = cq_raw.at[core * n_dq + index]
        return remote(blk, blk, cq_send.at[index], cq_recv.at[index])

    def dq_step(index, carry):
        dq_copy(index).wait()
        cq_raw[core * n_dq + index] = jnp.dot(a_chip[...], dq_buf[index], preferred_element_type=jnp.float32)
        cq_copy(index).start()
        return carry

    lax.fori_loop(0, n_dq, dq_step, 0)

    uk_copy.wait()
    for index in range(my_heads // SWAP_BLOCK):
        sel = slice(index * SWAP_BLOCK, (index + 1) * SWAP_BLOCK)
        wuk_buf[index] = jnp.swapaxes(uk_buf[:, sel, :], 0, 1)

    for index in range(n_dq):
        cq_copy(index).wait()
    total_sq = jnp.zeros((2 * rows, 1), jnp.float32)
    for index in range(2 * n_dq):
        vals = cq_raw[index]
        total_sq += jnp.sum(vals * vals, axis=-1, keepdims=True)
    inv = lax.rsqrt(total_sq * (1.0 / q_rank) + EPSILON)
    for index in range(2 * n_dq):
        for lane in range(0, DQ_W, 128):
            start = index * DQ_W + lane
            gain = gain_q_ref[start // 128:start // 128 + 1, :]
            cq_chip[:, start:start + 128] = (cq_raw[index, :, lane:lane + 128] * inv * gain).astype(jnp.bfloat16)

    cos_own, sin_own = cos_ref[...].T, sin_ref[...].T
    cos_far, sin_far = cs_recv[0].T, cs_recv[1].T
    first = core == 0
    cos_t = jnp.concatenate([jnp.where(first, cos_own, cos_far), jnp.where(first, cos_far, cos_own)], axis=0)
    sin_t = jnp.concatenate([jnp.where(first, sin_own, sin_far), jnp.where(first, sin_far, sin_own)], axis=0)

    def head_cols(index):
        return pl.ds(pl.multiple_of(core * my_heads + index * SWAP_BLOCK, SWAP_BLOCK), SWAP_BLOCK)

    def abs_copy(index):
        return remote(abs_part.at[index, other], abs_ref.at[:, head_cols(index), :], abs_send.at[index], abs_recv.at[index])

    def pe_copy(index):
        return remote(pe_part.at[index, other], pe_ref.at[:, head_cols(index), :], pe_send.at[index], pe_recv.at[index])

    def abs_keep(index):
        return pltpu.make_async_copy(abs_part.at[index, own], abs_ref.at[:, head_cols(index), :], keep_sem.at[0, index])

    def pe_keep(index):
        return pltpu.make_async_copy(pe_part.at[index, own], pe_ref.at[:, head_cols(index), :], keep_sem.at[1, index])

    per_swap = SWAP_BLOCK // HEAD_BLOCK

    def uq_step(index, carry):
        absorbed = []
        turned = []
        for sub in range(per_swap):
            uq_copy(index * per_swap + sub).wait()
        for sub in range(per_swap):
            q_val = lax.dot_general(cq_chip[...], uq_buf[index * per_swap + sub], NT, preferred_element_type=jnp.float32)
            for head in range(HEAD_BLOCK):
                base = head * head_dim
                nope = q_val[:, base:base + nope_dim].astype(jnp.bfloat16)
                low_half = q_val[:, base + nope_dim:base + nope_dim + half_dim]
                high_half = q_val[:, base + nope_dim + half_dim:base + head_dim]
                turned.append(jnp.concatenate([low_half * cos_t - high_half * sin_t, high_half * cos_t + low_half * sin_t], axis=1).astype(jnp.bfloat16))
                absorbed.append(lax.dot_general(nope, wuk_buf[index, sub * HEAD_BLOCK + head], NT, preferred_element_type=jnp.float32).astype(jnp.bfloat16))
        abs_part[index] = jnp.swapaxes(jnp.stack(absorbed, axis=0), 0, 1)
        pe_part[index] = jnp.swapaxes(jnp.stack(turned, axis=0), 0, 1)
        for move in (abs_copy, pe_copy, abs_keep, pe_keep):
            move(index).start()
        return carry

    n_swap = n_uq // per_swap
    lax.fori_loop(0, n_swap, uq_step, 0)

    dkv_copy.wait()
    kv_part[...] = lax.dot_general(a_chip[:, my_k], dkv_buf[...], NT, preferred_element_type=jnp.float32)
    kv_copy = remote(kv_part.at[other, :], kv_recv, kv_send, kv_got)
    kv_copy.start()
    kv_copy.wait()
    kv_val = kv_part[own, :] + kv_recv[...]
    latent = kv_val[:, :latent_dim]
    inv = lax.rsqrt(jnp.mean(latent * latent, axis=-1, keepdims=True) + EPSILON)
    ckv_ref[...] = (latent * inv * gain_kv_ref[...]).astype(jnp.bfloat16)
    low_half = kv_val[:, latent_dim:latent_dim + half_dim]
    high_half = kv_val[:, latent_dim + half_dim:]
    kpe_ref[...] = jnp.concatenate([low_half * cos_own - high_half * sin_own, high_half * cos_own + low_half * sin_own], axis=1).astype(jnp.bfloat16)
    for index in range(n_swap):
        for move in (abs_copy, pe_copy, abs_keep, pe_keep):
            move(index).wait()


def front(hidden, norm_attn, w_dq, norm_q, w_uq, w_dkv, norm_kv, w_uk, rope_cos, rope_sin):
    rows, d_model = hidden.shape
    latent_dim, heads, nope_dim = w_uk.shape
    q_rank, _, head_dim = w_uq.shape
    rope_dim = head_dim - nope_dim
    half_dim = rope_dim // 2
    kv_dim = w_dkv.shape[1]
    n_dq = q_rank // 2 // DQ_W
    n_uq = heads // 2 // HEAD_BLOCK
    n_swap = heads // 2 // SWAP_BLOCK
    f32, bf16 = jnp.float32, jnp.bfloat16
    vmem = pl.BlockSpec(memory_space=pltpu.VMEM)
    anywhere = pl.BlockSpec(memory_space=pl.ANY)
    dma = pltpu.SemaphoreType.DMA
    return pl.pallas_call(
        front_kernel,
        out_shape=[
            jax.ShapeDtypeStruct((rows, heads, latent_dim), bf16),
            jax.ShapeDtypeStruct((rows, heads, rope_dim), bf16),
            jax.ShapeDtypeStruct((rows, latent_dim), bf16),
            jax.ShapeDtypeStruct((rows, rope_dim), bf16),
        ],
        in_specs=[anywhere] + [vmem] * 5 + [anywhere] * 4,
        out_specs=[anywhere, anywhere, vmem, vmem],
        scratch_shapes=[
            pltpu.VMEM((n_dq, d_model, DQ_W), bf16),
            pltpu.VMEM((kv_dim, d_model // 2), bf16),
            pltpu.VMEM((n_uq, HEAD_BLOCK * head_dim, q_rank), bf16),
            pltpu.VMEM((latent_dim, heads // 2, nope_dim), bf16),
            pltpu.VMEM((n_swap, SWAP_BLOCK, latent_dim, nope_dim), bf16),
            pltpu.VMEM((rows, d_model), bf16),
            pltpu.VMEM((rows, d_model), bf16),
            pltpu.VMEM((2, half_dim, rows), f32),
            pltpu.VMEM((2 * rows, d_model), bf16),
            pltpu.VMEM((2 * n_dq, 2 * rows, DQ_W), f32),
            pltpu.VMEM((2 * rows, q_rank), bf16),
            pltpu.VMEM((2 * rows, kv_dim), f32),
            pltpu.VMEM((rows, kv_dim), f32),
            pltpu.VMEM((n_swap, 2 * rows, SWAP_BLOCK, latent_dim), bf16),
            pltpu.VMEM((n_swap, 2 * rows, SWAP_BLOCK, rope_dim), bf16),
            pltpu.VMEM((rows, 1), f32),
            dma(()), dma((n_dq,)), dma(()), dma((n_uq,)), dma(()), dma((3,)), dma((3,)), dma((n_dq,)), dma((n_dq,)), dma(()), dma(()),
            dma((n_swap,)), dma((n_swap,)), dma((n_swap,)), dma((n_swap,)), dma((2, n_swap)),
        ],
        compiler_params=pltpu.CompilerParams(collective_id=1, has_side_effects=True, vmem_limit_bytes=66 * 1000 * 1000),
        name='front',
    )(hidden, norm_attn.reshape(1, -1), norm_q.reshape(-1, 128), norm_kv.reshape(1, -1), rope_cos.T, rope_sin.T,
      w_dq, w_dkv.T, jnp.transpose(w_uq, (1, 2, 0)).reshape(heads * head_dim, q_rank), w_uk)


def attention_rows(hidden, ckv_cache, kpe_cache, cache_len, rope_cos, rope_sin, norm_attn, w_dq, norm_q, w_uq, w_dkv, norm_kv, w_uk, w_uv):
    score_scale = MSCALE * MSCALE / math.sqrt(w_uq.shape[2])
    q_abs, q_pe, ckv_new, kpe_new = front(hidden, norm_attn, w_dq, norm_q, w_uq, w_dkv, norm_kv, w_uk, rope_cos, rope_sin)
    head_out, ckv_new, kpe_new = attend(q_abs, q_pe, ckv_new, kpe_new, ckv_cache, kpe_cache, cache_len, w_uv, score_scale)
    return head_out, ckv_new, kpe_new


def tail_kernel(o_ref, x_ref, gain_ref, wout_ref, wgate_ref, wup_ref, wdown_ref, out_ref,
                slots, o_chip, x_chip, x_own, r_all, u_all, gate_buf, up_buf, act, sq_acc, pair_send, pair_recv, far_send, far_recv, own_sum, out_buf,
                slot_sem, in_send, in_recv, loc_sem, rp_send, rp_recv, rx_send, rx_recv, rf_send, rf_recv,
                pp_send, pp_recv, px_send, px_recv, out_sem):
    rep, me, chip, core = _sides()
    part = chip * 2 + (1 - core)
    opp = (1 - chip) * 2 + core
    diag = (1 - chip) * 2 + (1 - core)
    attn_k = wout_ref.shape[0]
    d_model = wgate_ref.shape[0]
    ff = wgate_ref.shape[1]
    rows = x_ref.shape[0]
    half = d_model // 2
    n_out = half // OUT_W
    n_ff = ff // OUT_W
    n_down = d_model // OUT_W
    first_ff = n_out
    first_down = n_out + 2 * n_ff
    total = first_down + n_down
    pieces = OUT_W // PIECE
    n_half = half // PIECE
    n_all = d_model // PIECE

    def col(index):
        return pl.ds(pl.multiple_of(index * OUT_W, OUT_W), OUT_W)

    def piece(index):
        return pl.ds(pl.multiple_of(index * PIECE, PIECE), PIECE)

    def row_block(owner, count=1):
        return pl.ds(pl.multiple_of(owner * rows, rows), count * rows)

    def slot_copy(kind, index, step):
        slot = lax.rem(step, SLOTS)
        src = {'out': wout_ref, 'gate': wgate_ref, 'up': wup_ref, 'down': wdown_ref}[kind]
        depth = src.shape[0]
        return pltpu.make_async_copy(src.at[:, col(index)], slots.at[slot, pl.ds(0, depth), :], slot_sem.at[slot])

    def fetch(step):
        @pl.when(step < first_ff)
        def _():
            slot_copy('out', core * n_out + step, step).start()

        @pl.when((step >= first_ff) & (step < first_down) & (lax.rem(step - first_ff, 2) == 0))
        def _():
            slot_copy('gate', (step - first_ff) // 2, step).start()

        @pl.when((step >= first_ff) & (step < first_down) & (lax.rem(step - first_ff, 2) == 1))
        def _():
            slot_copy('up', (step - first_ff) // 2, step).start()

        @pl.when((step >= first_down) & (step < total))
        def _():
            slot_copy('down', step - first_down, step).start()

    my_rows = row_block(core)
    my_half = pl.ds(pl.multiple_of(core * half, half), half)
    their_half = pl.ds(pl.multiple_of((1 - core) * half, half), half)
    keep_o = pltpu.make_async_copy(o_ref, o_chip.at[my_rows, :], loc_sem.at[0])
    keep_x = pltpu.make_async_copy(x_ref.at[:, my_half], x_chip.at[my_rows, :], loc_sem.at[1])
    give_x = pltpu.make_async_copy(x_ref.at[:, their_half], x_own, loc_sem.at[2])
    keep_o.start()
    give_x.start()
    keep_x.start()
    slot_copy('out', core * n_out, 0).start()

    barrier = pltpu.get_barrier_semaphore()
    for peer in (part, opp):
        pl.semaphore_signal(barrier, inc=1, device_id=(rep, peer), device_id_type=MESH)
    pl.semaphore_wait(barrier, 2)

    def remote(src, dst, send, recv, peer):
        return pltpu.make_async_remote_copy(src_ref=src, dst_ref=dst, send_sem=send, recv_sem=recv,
                                            device_id=(rep, peer), device_id_type=MESH)

    keep_o.wait()
    send_o = remote(o_chip.at[my_rows, :], o_chip.at[my_rows, :], in_send.at[0], in_recv.at[0], part)
    send_o.start()
    give_x.wait()
    send_x = remote(x_own, x_chip.at[my_rows, :], in_send.at[1], in_recv.at[1], part)
    send_x.start()
    for step in range(1, SLOTS):
        slot_copy('out', core * n_out + step, step).start()
    sq_acc[...] = jnp.zeros_like(sq_acc)
    gate_buf[...] = jnp.zeros_like(gate_buf)
    up_buf[...] = jnp.zeros_like(up_buf)
    keep_x.wait()
    send_o.wait()
    send_x.wait()

    chip_rows = row_block(chip * 2, 2)
    far_rows = row_block((1 - chip) * 2, 2)

    def r_pair(index):
        blk = r_all.at[core * n_half + index, chip_rows, :]
        return remote(blk, blk, rp_send.at[index], rp_recv.at[index], part)

    def r_far(index):
        blk = r_all.at[core * n_half + index, chip_rows, :]
        return remote(blk, blk, rx_send.at[index], rx_recv.at[index], opp)

    def r_forward(index):
        blk = r_all.at[core * n_half + index, far_rows, :]
        return remote(blk, blk, rf_send.at[index], rf_recv.at[index], part)

    def add_squares(sel, vals):
        wide = vals.astype(jnp.float32)
        wide = wide * wide
        acc = sq_acc[sel, :]
        for lane in range(0, PIECE, 128):
            acc = acc + wide[:, lane:lane + 128]
        sq_acc[sel, :] = acc

    def take_pair(index):
        r_pair(index).wait_recv()
        add_squares(chip_rows, r_all[(1 - core) * n_half + index, chip_rows, :])

    def take_far(index):
        r_far(index).wait_recv()
        r_forward(index).start()
        add_squares(far_rows, r_all[core * n_half + index, far_rows, :])

    def take_forward(index):
        r_forward(index).wait_recv()
        add_squares(far_rows, r_all[(1 - core) * n_half + index, far_rows, :])

    lags = ((take_pair, 2), (take_far, 4), (take_forward, 6))

    def out_step(index, carry):
        slot_copy('out', core * n_out + index, index).wait()
        for sub in range(pieces):
            here = index * pieces + sub
            acc = jnp.dot(o_chip[...], slots[lax.rem(index, SLOTS), :attn_k, sub * PIECE:(sub + 1) * PIECE], preferred_element_type=jnp.float32)
            vals = (x_chip[:, piece(here)].astype(jnp.float32) + acc).astype(jnp.bfloat16)
            r_all[core * n_half + here, chip_rows, :] = vals
            r_far(here).start()
            r_pair(here).start()
            add_squares(chip_rows, vals)
            for take, lag in lags:
                @pl.when(here >= lag)
                def _(take=take, lag=lag):
                    take(here - lag)
        fetch(index + SLOTS)
        return carry

    lax.fori_loop(0, n_out, out_step, 0)

    def inverse(owner):
        total_sq = jnp.sum(sq_acc[row_block(owner), :], axis=-1, keepdims=True)
        return lax.rsqrt(total_sq * (1.0 / d_model) + EPSILON)

    def normalise(places):
        invs = [inverse(owner) for _, owner in places]

        def norm_step(index, carry):
            for (place, owner), inv in zip(places, carry):
                vals = r_all[index, row_block(owner), :].astype(jnp.float32) * inv * gain_ref[0:1, piece(index)]
                u_all[place * rows:(place + 1) * rows, piece(index)] = vals.astype(jnp.bfloat16)
            return carry

        lax.fori_loop(0, n_all, norm_step, tuple(invs))

    for index in range(n_half - 2, n_half):
        take_pair(index)
    take_far(n_half - 4)
    take_forward(n_half - 6)
    take_far(n_half - 3)
    take_forward(n_half - 5)
    normalise(((0, part), (1, me)))
    near = slice(0, 2 * rows)
    far = slice(2 * rows, 4 * rows)

    def activate(gate_val, up_val):
        return (gate_val * jax.nn.sigmoid(gate_val) * up_val).astype(jnp.bfloat16)

    def product(sel, step):
        return jnp.dot(u_all[sel, :], slots[lax.rem(step, SLOTS), :d_model, :], preferred_element_type=jnp.float32)

    def early(index, sel):
        step = first_ff + 2 * index
        gate_val = product(sel, step)
        act[sel, index * OUT_W:(index + 1) * OUT_W] = activate(gate_val, product(sel, step + 1))

    for index in range(EARLY):
        slot_copy('gate', index, first_ff + 2 * index).wait()
        slot_copy('up', index, first_ff + 2 * index + 1).wait()
        early(index, near)
        if index == 0:
            take_far(n_half - 2)
            take_far(n_half - 1)
            take_forward(n_half - 4)
            take_forward(n_half - 3)
    take_forward(n_half - 2)
    take_forward(n_half - 1)
    normalise(((2, diag), (3, opp)))
    for index in range(EARLY):
        early(index, far)
        fetch(first_ff + 2 * index + SLOTS)
        fetch(first_ff + 2 * index + 1 + SLOTS)

    def ff_step(index, carry):
        step = first_ff + 2 * index
        now, before = lax.rem(index, 2), lax.rem(index + 1, 2)
        slot_copy('gate', index, step).wait()
        act[:, col(jnp.maximum(index - 1, EARLY))] = activate(gate_buf[before], up_buf[...])
        gate_buf[now] = product(slice(None), step)
        fetch(step + SLOTS)
        slot_copy('up', index, step + 1).wait()
        up_buf[...] = product(slice(None), step + 1)
        fetch(step + 1 + SLOTS)
        return carry

    lax.fori_loop(EARLY, n_ff, ff_step, 0)
    act[:, (n_ff - 1) * OUT_W:] = activate(gate_buf[(n_ff - 1) % 2], up_buf[...])

    def pair_copy(index):
        return remote(pair_send.at[index], pair_recv.at[index], pp_send.at[index], pp_recv.at[index], part)

    def far_copy(index):
        return remote(far_send.at[index], far_recv.at[index], px_send.at[index], px_recv.at[index], opp)

    def combine(index):
        pair_copy(index).wait_recv()
        far_send[index] += pair_recv[index, rows:, :]
        far_copy(index).start()
        own_sum[index] += pair_recv[index, :rows, :]

    def down_step(index, carry):
        step = first_down + index
        slot_copy('down', index, step).wait()
        for sub in range(pieces):
            here = index * pieces + sub
            part_sum = jnp.dot(act[...], slots[lax.rem(step, SLOTS), :ff, sub * PIECE:(sub + 1) * PIECE], preferred_element_type=jnp.float32)
            pair_send[here, :rows] = part_sum[:rows]
            pair_send[here, rows:] = part_sum[2 * rows:3 * rows]
            own_sum[here] = part_sum[rows:2 * rows]
            far_send[here] = part_sum[3 * rows:]
            pair_copy(here).start()

            @pl.when(here >= 1)
            def _():
                combine(here - 1)
        fetch(step + SLOTS)
        return carry

    lax.fori_loop(0, n_down, down_step, 0)
    combine(n_all - 1)

    def settle(index, carry):
        r_pair(index).wait_send()
        r_far(index).wait_send()
        r_forward(index).wait_send()
        return carry

    lax.fori_loop(0, n_half, settle, 0)
    own_rows = row_block(me)

    def out_copy(index):
        return pltpu.make_async_copy(out_buf.at[:, piece(index)], out_ref.at[:, piece(index)], out_sem.at[index])

    def finish(index, carry):
        far_copy(index).wait()
        pair_copy(index).wait_send()
        mlp = own_sum[index] + far_recv[index]
        out_buf[:, piece(index)] = (r_all[index, own_rows, :].astype(jnp.float32) + mlp).astype(jnp.bfloat16)
        out_copy(index).start()
        return carry

    lax.fori_loop(0, n_all, finish, 0)

    def flush(index, carry):
        out_copy(index).wait()
        return carry

    lax.fori_loop(0, n_all, flush, 0)


def tail(head_out, hidden, norm_mlp, w_out, w_gate, w_up, w_down):
    rows, d_model = hidden.shape
    attn_k = w_out.shape[0]
    ff = w_gate.shape[1]
    n_half = d_model // 2 // PIECE
    n_all = d_model // PIECE
    depth = max(attn_k, d_model, ff)
    vmem = pl.BlockSpec(memory_space=pltpu.VMEM)
    anywhere = pl.BlockSpec(memory_space=pl.ANY)
    dma = pltpu.SemaphoreType.DMA
    f32, bf16 = jnp.float32, jnp.bfloat16
    return pl.pallas_call(
        tail_kernel,
        out_shape=jax.ShapeDtypeStruct((rows, d_model), bf16),
        in_specs=[anywhere, anywhere, vmem, anywhere, anywhere, anywhere, anywhere],
        out_specs=anywhere,
        scratch_shapes=[
            pltpu.VMEM((SLOTS, depth, OUT_W), bf16),
            pltpu.VMEM((2 * rows, attn_k), bf16),
            pltpu.VMEM((2 * rows, d_model // 2), bf16),
            pltpu.VMEM((rows, d_model // 2), bf16),
            pltpu.VMEM((n_all, 4 * rows, PIECE), bf16),
            pltpu.VMEM((4 * rows, d_model), bf16),
            pltpu.VMEM((2, 4 * rows, OUT_W), f32),
            pltpu.VMEM((4 * rows, OUT_W), f32),
            pltpu.VMEM((4 * rows, ff), bf16),
            pltpu.VMEM((4 * rows, 128), f32),
            pltpu.VMEM((n_all, 2 * rows, PIECE), f32),
            pltpu.VMEM((n_all, 2 * rows, PIECE), f32),
            pltpu.VMEM((n_all, rows, PIECE), f32),
            pltpu.VMEM((n_all, rows, PIECE), f32),
            pltpu.VMEM((n_all, rows, PIECE), f32),
            pltpu.VMEM((rows, d_model), bf16),
            dma((SLOTS,)), dma((2,)), dma((2,)), dma((3,)),
            dma((n_half,)), dma((n_half,)), dma((n_half,)), dma((n_half,)), dma((n_half,)), dma((n_half,)),
            dma((n_all,)), dma((n_all,)), dma((n_all,)), dma((n_all,)), dma((n_all,)),
        ],
        compiler_params=pltpu.CompilerParams(collective_id=0, has_side_effects=True, vmem_limit_bytes=66 * 1000 * 1000),
        name='tail',
    )(head_out, hidden, norm_mlp.reshape(1, d_model), w_out, w_gate, w_up, w_down)


def solution(mesh):
    row_spec = P(('rep', 'dp'), None)
    cube_spec = P(('rep', 'dp'), None, None)
    full_spec = P()
    in_specs = (row_spec, cube_spec, cube_spec, P(('rep', 'dp')), row_spec, row_spec,
                full_spec, full_spec, full_spec, full_spec, full_spec, full_spec, full_spec, full_spec, full_spec, full_spec,
                P(None, 'dp'), P(None, 'dp'), P('dp', None))

    def local_step(hidden, ckv_cache, kpe_cache, cache_len, rope_cos, rope_sin, norm_attn, w_dq, norm_q, w_uq, w_dkv, norm_kv, w_uk, w_uv, w_out, norm_mlp, w_gate, w_up, w_down):
        head_out, ckv_new, kpe_new = attention_rows(hidden, ckv_cache, kpe_cache, cache_len, rope_cos, rope_sin, norm_attn, w_dq, norm_q, w_uq, w_dkv, norm_kv, w_uk, w_uv)
        out_hidden = tail(head_out, hidden, norm_mlp, w_out.reshape(-1, w_out.shape[-1]), w_gate, w_up, w_down)
        return out_hidden, ckv_new, kpe_new

    return jax.shard_map(local_step, mesh=mesh, in_specs=in_specs, out_specs=(row_spec, row_spec, row_spec), check_vma=False)
```

```python
import functools
import math
import jax
import jax.numpy as jnp
from jax import lax
from jax.experimental import pallas as pl
from jax.experimental.pallas import tpu as pltpu
from jax.sharding import PartitionSpec as P

EPSILON = 1e-6
MSCALE = 0.1 * math.log(40.0) + 1.0
MESH = pl.DeviceIdType.MESH


OUT_W = 512
PIECE = 256
SLOTS = 4
EARLY = 1
HEAD_BLOCK = 8
SWAP_BLOCK = 16
NT = (((1,), (1,)), ((), ()))
NN = (((1,), (0,)), ((), ()))


GROUP = 8
BUFFERS = 3
CHUNK = 128


def attend_kernel(score_scale, len_ref, abs_hbm, pe_hbm, new_ref, pe_new_ref, ckv_ref, kpe_ref, wuv_ref,
                  out_ref, new_out_ref, pe_out_ref, order_buf, turned_buf, abs_ref, pe_ref, kv_buf, kp_buf, lat_buf, wuv_buf, kv_sem, kp_sem, wuv_sem, query_sem):
    query_copies = [pltpu.make_async_copy(abs_hbm, abs_ref, query_sem.at[0]), pltpu.make_async_copy(pe_hbm, pe_ref, query_sem.at[1])]
    for made in query_copies:
        made.start()
    rows, heads, latent_dim = abs_ref.shape
    seq = ckv_ref.shape[1]
    variants = seq // CHUNK
    groups = rows // GROUP
    value_dim = wuv_ref.shape[2]

    def chunks_of(row):
        return len_ref[row] // CHUNK

    def count_step(row, tally):
        return tuple(count + (chunks_of(row) == which).astype(jnp.int32) for which, count in enumerate(tally))

    tally = lax.fori_loop(0, rows, count_step, (jnp.int32(0),) * variants)
    starts = [jnp.int32(0)]
    for which in range(variants - 1):
        starts.append(starts[-1] + tally[which])

    def place_step(row, heads_of):
        mine = [chunks_of(row) == which for which in range(variants)]
        place = sum(jnp.where(hit, head, 0) for hit, head in zip(mine, heads_of))
        order_buf[place] = row
        return tuple(head + hit.astype(jnp.int32) for hit, head in zip(mine, heads_of))

    lax.fori_loop(0, rows, place_step, tuple(starts))

    def group_chunks(group):
        return chunks_of(order_buf[group * GROUP + GROUP - 1]) + 1

    def copies(group, size):
        slot = lax.rem(group, BUFFERS)
        made = []
        for place in range(GROUP):
            row = order_buf[group * GROUP + place]
            made.append(pltpu.make_async_copy(ckv_ref.at[row, pl.ds(0, size), :], kv_buf.at[slot, place, pl.ds(0, size), :], kv_sem.at[slot, place]))
            made.append(pltpu.make_async_copy(kpe_ref.at[row, :, pl.ds(0, size)], kp_buf.at[slot, place, :, pl.ds(0, size)], kp_sem.at[slot, place]))
        return made

    def start(group):
        for count in range(1, variants + 1):
            @pl.when(group_chunks(group) == count)
            def _():
                for made in copies(group, count * CHUNK):
                    made.start()

    for group in range(BUFFERS - 1):
        start(group)
    wuv_copy = pltpu.make_async_copy(wuv_ref, wuv_buf, wuv_sem)
    turned_buf[...] = pe_new_ref[...].astype(jnp.float32).T
    new_out_ref[...] = new_ref[...]
    pe_out_ref[...] = pe_new_ref[...]

    def compute(group, size):
        slot = lax.rem(group, BUFFERS)
        for made in copies(group, size):
            made.wait()
        rows_of = [order_buf[group * GROUP + place] for place in range(GROUP)]
        for place, row in enumerate(rows_of):
            length = len_ref[row]
            base = pl.multiple_of((row // 16) * 16, 16)
            picked = new_ref[pl.ds(base, 16), :].astype(jnp.float32)
            hit = lax.broadcasted_iota(jnp.int32, picked.shape, 0) == row - base
            new = jnp.sum(jnp.where(hit, picked, 0.0), axis=0, keepdims=True)
            hit = lax.broadcasted_iota(jnp.int32, turned_buf.shape, 1) == row
            new_pe = jnp.sum(jnp.where(hit, turned_buf[...], 0.0), axis=1, keepdims=True)
            base = pl.multiple_of((length // 16) * 16, 16)
            block = kv_buf[slot, place, pl.ds(base, 16), :]
            hit = lax.broadcasted_iota(jnp.int32, block.shape, 0) == length - base
            kv_buf[slot, place, pl.ds(base, 16), :] = jnp.where(hit, new, block.astype(jnp.float32)).astype(jnp.bfloat16)
            lane = pl.multiple_of((length // CHUNK) * CHUNK, CHUNK)
            block = kp_buf[slot, place, :, pl.ds(lane, CHUNK)]
            hit = lax.broadcasted_iota(jnp.int32, block.shape, 1) == length - lane
            kp_buf[slot, place, :, pl.ds(lane, CHUNK)] = jnp.where(hit, new_pe, block.astype(jnp.float32)).astype(jnp.bfloat16)
        all_scores = [(lax.dot_general(abs_ref[row], kv_buf[slot, place, :size, :], NT, preferred_element_type=jnp.float32)
                       + jnp.dot(pe_ref[row], kp_buf[slot, place, :, :size], preferred_element_type=jnp.float32)) * score_scale
                      for place, row in enumerate(rows_of)]
        weights = []
        for place, row in enumerate(rows_of):
            positions = lax.broadcasted_iota(jnp.int32, (heads, size), 1)
            scores = jnp.where(positions <= len_ref[row], all_scores[place], -jnp.inf)
            exp_all = jnp.exp(scores - jnp.max(scores, axis=1, keepdims=True))
            weights.append((exp_all.astype(jnp.bfloat16), jnp.sum(exp_all, axis=1, keepdims=True)))
        for place, row in enumerate(rows_of):
            weighted = jnp.dot(weights[place][0], kv_buf[slot, place, :size, :], preferred_element_type=jnp.float32)
            lat_buf[row] = (weighted / weights[place][1]).astype(jnp.bfloat16)

    def group_step(group, carry):
        @pl.when(group == groups - 3)
        def _():
            wuv_copy.start()

        @pl.when(group + BUFFERS - 1 < groups)
        def _():
            start(group + BUFFERS - 1)
        for count in range(1, variants + 1):
            @pl.when(group_chunks(group) == count)
            def _():
                compute(group, count * CHUNK)
        return carry

    for made in query_copies:
        made.wait()
    lax.fori_loop(0, groups, group_step, 0)
    wuv_copy.wait()

    def value_step(block, carry):
        sel = pl.ds(pl.multiple_of(block * SWAP_BLOCK, SWAP_BLOCK), SWAP_BLOCK)
        lat = jnp.swapaxes(lat_buf[:, sel, :], 0, 1)
        wuv = jnp.swapaxes(wuv_buf[:, sel, :], 0, 1)
        for head in range(SWAP_BLOCK):
            dst = pl.ds(pl.multiple_of(block * SWAP_BLOCK * value_dim + head * value_dim, value_dim), value_dim)
            out_ref[:, dst] = jnp.dot(lat[head], wuv[head], preferred_element_type=jnp.float32).astype(jnp.bfloat16)
        return carry

    lax.fori_loop(0, heads // SWAP_BLOCK, value_step, 0)


def attend(q_abs, q_pe, ckv_new, kpe_new, ckv_cache, kpe_cache, cache_len, w_uv, score_scale):
    rows, heads, latent_dim = q_abs.shape
    rope_dim = q_pe.shape[2]
    seq = ckv_cache.shape[1]
    value_dim = w_uv.shape[2]
    smem = pl.BlockSpec(memory_space=pltpu.SMEM)
    vmem = pl.BlockSpec(memory_space=pltpu.VMEM)
    anywhere = pl.BlockSpec(memory_space=pl.ANY)
    dma = pltpu.SemaphoreType.DMA
    return pl.pallas_call(
        functools.partial(attend_kernel, score_scale),
        out_shape=[jax.ShapeDtypeStruct((rows, heads * value_dim), jnp.bfloat16),
                   jax.ShapeDtypeStruct(ckv_new.shape, jnp.bfloat16), jax.ShapeDtypeStruct(kpe_new.shape, jnp.bfloat16)],
        in_specs=[smem, anywhere, anywhere, vmem, vmem, anywhere, anywhere, anywhere],
        out_specs=[vmem, vmem, vmem],
        scratch_shapes=[
            pltpu.SMEM((rows,), jnp.int32),
            pltpu.VMEM((rope_dim, rows), jnp.float32),
            pltpu.VMEM(q_abs.shape, jnp.bfloat16),
            pltpu.VMEM(q_pe.shape, jnp.bfloat16),
            pltpu.VMEM((BUFFERS, GROUP, seq, latent_dim), jnp.bfloat16),
            pltpu.VMEM((BUFFERS, GROUP, rope_dim, seq), jnp.bfloat16),
            pltpu.VMEM((rows, heads, latent_dim), jnp.bfloat16),
            pltpu.VMEM(w_uv.shape, jnp.bfloat16),
            dma((BUFFERS, GROUP)), dma((BUFFERS, GROUP)), dma(()), dma((2,)),
        ],
        compiler_params=pltpu.CompilerParams(vmem_limit_bytes=60 * 1000 * 1000),
        name='attend',
    )(cache_len, q_abs, q_pe, ckv_new, kpe_new, ckv_cache, jnp.swapaxes(kpe_cache, 1, 2), w_uv)


DQ_W = 256


def _sides():
    rep = lax.axis_index('rep')
    me = lax.axis_index('dp')
    chip = me // 2
    core = lax.rem(me, 2)
    return rep, me, chip, core


def front_kernel(x_ref, gain_ref, gain_q_ref, gain_kv_ref, cos_ref, sin_ref, wdq_ref, wdkv_ref, wuq_ref, wuk_ref,
                 abs_ref, pe_ref, ckv_ref, kpe_ref,
                 dq_buf, dkv_buf, uq_buf, uk_buf, wuk_buf, x_own, x_recv, cs_recv, a_chip, cq_raw, cq_chip, kv_part, kv_recv, abs_part, pe_part, stat,
                 x_sem, dq_sem, dkv_sem, uq_sem, uk_sem, in_send, in_recv, cq_send, cq_recv, kv_send, kv_got, abs_send, abs_recv, pe_send, pe_recv, keep_sem):
    rep, me, chip, core = _sides()
    part = chip * 2 + (1 - core)
    rows, d_model = x_ref.shape
    latent_dim = ckv_ref.shape[1]
    rope_dim = kpe_ref.shape[1]
    half_dim = rope_dim // 2
    nope_dim = wuk_ref.shape[2]
    head_dim = nope_dim + rope_dim
    half_k = d_model // 2
    n_dq = dq_buf.shape[0]
    n_uq = uq_buf.shape[0]
    q_rank = cq_chip.shape[1]
    block_rows = HEAD_BLOCK * head_dim
    my_heads = n_uq * HEAD_BLOCK

    def dq_copy(index):
        cols = pl.ds(pl.multiple_of((core * n_dq + index) * DQ_W, DQ_W), DQ_W)
        return pltpu.make_async_copy(wdq_ref.at[:, cols], dq_buf.at[index], dq_sem.at[index])

    def uq_copy(index):
        sel = pl.ds(pl.multiple_of((core * n_uq + index) * block_rows, block_rows), block_rows)
        return pltpu.make_async_copy(wuq_ref.at[sel, :], uq_buf.at[index], uq_sem.at[index])

    my_k = pl.ds(pl.multiple_of(core * half_k, half_k), half_k)
    dkv_copy = pltpu.make_async_copy(wdkv_ref.at[:, my_k], dkv_buf, dkv_sem)
    heads_here = pl.ds(pl.multiple_of(core * my_heads, my_heads), my_heads)
    uk_copy = pltpu.make_async_copy(wuk_ref.at[:, heads_here, :], uk_buf, uk_sem)
    x_copy = pltpu.make_async_copy(x_ref, x_own, x_sem)
    x_copy.start()
    dq_copy(0).start()

    barrier = pltpu.get_barrier_semaphore()
    pl.semaphore_signal(barrier, inc=1, device_id=(rep, part), device_id_type=MESH)
    pl.semaphore_wait(barrier, 1)

    def remote(src, dst, send, recv):
        return pltpu.make_async_remote_copy(src_ref=src, dst_ref=dst, send_sem=send, recv_sem=recv,
                                            device_id=(rep, part), device_id_type=MESH)

    x_copy.wait()
    swaps = [remote(x_own, x_recv, in_send.at[0], in_recv.at[0]),
             remote(cos_ref, cs_recv.at[0], in_send.at[1], in_recv.at[1]),
             remote(sin_ref, cs_recv.at[1], in_send.at[2], in_recv.at[2])]
    for swap in swaps:
        swap.start()
    for index in range(1, n_dq):
        dq_copy(index).start()
    uk_copy.start()
    for index in range(n_uq):
        uq_copy(index).start()
    dkv_copy.start()

    own = pl.ds(pl.multiple_of(core * rows, rows), rows)
    other = pl.ds(pl.multiple_of((1 - core) * rows, rows), rows)
    n_cols = d_model // OUT_W

    def normalise(src_ref, dst_rows):
        def square_step(index, total_sq):
            vals = src_ref[:, pl.ds(pl.multiple_of(index * OUT_W, OUT_W), OUT_W)].astype(jnp.float32)
            return total_sq + jnp.sum(vals * vals, axis=-1, keepdims=True)

        total_sq = lax.fori_loop(0, n_cols, square_step, jnp.zeros((rows, 1), jnp.float32))
        stat[...] = lax.rsqrt(total_sq * (1.0 / d_model) + EPSILON)

        def scale_step(index, carry):
            cols = pl.ds(pl.multiple_of(index * OUT_W, OUT_W), OUT_W)
            vals = src_ref[:, cols].astype(jnp.float32) * stat[...] * gain_ref[0:1, cols]
            a_chip[dst_rows, cols] = vals.astype(jnp.bfloat16)
            return carry

        lax.fori_loop(0, n_cols, scale_step, 0)

    normalise(x_own, own)
    for swap in swaps:
        swap.wait()
    normalise(x_recv, other)

    def cq_copy(index):
        blk = cq_raw.at[core * n_dq + index]
        return remote(blk, blk, cq_send.at[index], cq_recv.at[index])

    def dq_step(index, carry):
        dq_copy(index).wait()
        cq_raw[core * n_dq + index] = jnp.dot(a_chip[...], dq_buf[index], preferred_element_type=jnp.float32)
        cq_copy(index).start()
        return carry

    lax.fori_loop(0, n_dq, dq_step, 0)

    uk_copy.wait()
    for index in range(my_heads // SWAP_BLOCK):
        sel = slice(index * SWAP_BLOCK, (index + 1) * SWAP_BLOCK)
        wuk_buf[index] = jnp.swapaxes(uk_buf[:, sel, :], 0, 1)

    for index in range(n_dq):
        cq_copy(index).wait()
    total_sq = jnp.zeros((2 * rows, 1), jnp.float32)
    for index in range(2 * n_dq):
        vals = cq_raw[index]
        total_sq += jnp.sum(vals * vals, axis=-1, keepdims=True)
    inv = lax.rsqrt(total_sq * (1.0 / q_rank) + EPSILON)
    for index in range(2 * n_dq):
        for lane in range(0, DQ_W, 128):
            start = index * DQ_W + lane
            gain = gain_q_ref[start // 128:start // 128 + 1, :]
            cq_chip[:, start:start + 128] = (cq_raw[index, :, lane:lane + 128] * inv * gain).astype(jnp.bfloat16)

    cos_own, sin_own = cos_ref[...].T, sin_ref[...].T
    cos_far, sin_far = cs_recv[0].T, cs_recv[1].T
    first = core == 0
    cos_t = jnp.concatenate([jnp.where(first, cos_own, cos_far), jnp.where(first, cos_far, cos_own)], axis=0)
    sin_t = jnp.concatenate([jnp.where(first, sin_own, sin_far), jnp.where(first, sin_far, sin_own)], axis=0)

    def head_cols(index):
        return pl.ds(pl.multiple_of(core * my_heads + index * SWAP_BLOCK, SWAP_BLOCK), SWAP_BLOCK)

    def abs_copy(index):
        return remote(abs_part.at[index, other], abs_ref.at[:, head_cols(index), :], abs_send.at[index], abs_recv.at[index])

    def pe_copy(index):
        return remote(pe_part.at[index, other], pe_ref.at[:, head_cols(index), :], pe_send.at[index], pe_recv.at[index])

    def abs_keep(index):
        return pltpu.make_async_copy(abs_part.at[index, own], abs_ref.at[:, head_cols(index), :], keep_sem.at[0, index])

    def pe_keep(index):
        return pltpu.make_async_copy(pe_part.at[index, own], pe_ref.at[:, head_cols(index), :], keep_sem.at[1, index])

    per_swap = SWAP_BLOCK // HEAD_BLOCK

    def uq_step(index, carry):
        absorbed = []
        turned = []
        for sub in range(per_swap):
            uq_copy(index * per_swap + sub).wait()
        for sub in range(per_swap):
            q_val = lax.dot_general(cq_chip[...], uq_buf[index * per_swap + sub], NT, preferred_element_type=jnp.float32)
            for head in range(HEAD_BLOCK):
                base = head * head_dim
                nope = q_val[:, base:base + nope_dim].astype(jnp.bfloat16)
                low_half = q_val[:, base + nope_dim:base + nope_dim + half_dim]
                high_half = q_val[:, base + nope_dim + half_dim:base + head_dim]
                turned.append(jnp.concatenate([low_half * cos_t - high_half * sin_t, high_half * cos_t + low_half * sin_t], axis=1).astype(jnp.bfloat16))
                absorbed.append(lax.dot_general(nope, wuk_buf[index, sub * HEAD_BLOCK + head], NT, preferred_element_type=jnp.float32).astype(jnp.bfloat16))
        abs_part[index] = jnp.swapaxes(jnp.stack(absorbed, axis=0), 0, 1)
        pe_part[index] = jnp.swapaxes(jnp.stack(turned, axis=0), 0, 1)
        for move in (abs_copy, pe_copy, abs_keep, pe_keep):
            move(index).start()
        return carry

    n_swap = n_uq // per_swap
    lax.fori_loop(0, n_swap, uq_step, 0)

    dkv_copy.wait()
    kv_part[...] = lax.dot_general(a_chip[:, my_k], dkv_buf[...], NT, preferred_element_type=jnp.float32)
    kv_copy = remote(kv_part.at[other, :], kv_recv, kv_send, kv_got)
    kv_copy.start()
    kv_copy.wait()
    kv_val = kv_part[own, :] + kv_recv[...]
    latent = kv_val[:, :latent_dim]
    inv = lax.rsqrt(jnp.mean(latent * latent, axis=-1, keepdims=True) + EPSILON)
    ckv_ref[...] = (latent * inv * gain_kv_ref[...]).astype(jnp.bfloat16)
    low_half = kv_val[:, latent_dim:latent_dim + half_dim]
    high_half = kv_val[:, latent_dim + half_dim:]
    kpe_ref[...] = jnp.concatenate([low_half * cos_own - high_half * sin_own, high_half * cos_own + low_half * sin_own], axis=1).astype(jnp.bfloat16)
    for index in range(n_swap):
        for move in (abs_copy, pe_copy, abs_keep, pe_keep):
            move(index).wait()


def front(hidden, norm_attn, w_dq, norm_q, w_uq, w_dkv, norm_kv, w_uk, rope_cos, rope_sin):
    rows, d_model = hidden.shape
    latent_dim, heads, nope_dim = w_uk.shape
    q_rank, _, head_dim = w_uq.shape
    rope_dim = head_dim - nope_dim
    half_dim = rope_dim // 2
    kv_dim = w_dkv.shape[1]
    n_dq = q_rank // 2 // DQ_W
    n_uq = heads // 2 // HEAD_BLOCK
    n_swap = heads // 2 // SWAP_BLOCK
    f32, bf16 = jnp.float32, jnp.bfloat16
    vmem = pl.BlockSpec(memory_space=pltpu.VMEM)
    anywhere = pl.BlockSpec(memory_space=pl.ANY)
    dma = pltpu.SemaphoreType.DMA
    return pl.pallas_call(
        front_kernel,
        out_shape=[
            jax.ShapeDtypeStruct((rows, heads, latent_dim), bf16),
            jax.ShapeDtypeStruct((rows, heads, rope_dim), bf16),
            jax.ShapeDtypeStruct((rows, latent_dim), bf16),
            jax.ShapeDtypeStruct((rows, rope_dim), bf16),
        ],
        in_specs=[anywhere] + [vmem] * 5 + [anywhere] * 4,
        out_specs=[anywhere, anywhere, vmem, vmem],
        scratch_shapes=[
            pltpu.VMEM((n_dq, d_model, DQ_W), bf16),
            pltpu.VMEM((kv_dim, d_model // 2), bf16),
            pltpu.VMEM((n_uq, HEAD_BLOCK * head_dim, q_rank), bf16),
            pltpu.VMEM((latent_dim, heads // 2, nope_dim), bf16),
            pltpu.VMEM((n_swap, SWAP_BLOCK, latent_dim, nope_dim), bf16),
            pltpu.VMEM((rows, d_model), bf16),
            pltpu.VMEM((rows, d_model), bf16),
            pltpu.VMEM((2, half_dim, rows), f32),
            pltpu.VMEM((2 * rows, d_model), bf16),
            pltpu.VMEM((2 * n_dq, 2 * rows, DQ_W), f32),
            pltpu.VMEM((2 * rows, q_rank), bf16),
            pltpu.VMEM((2 * rows, kv_dim), f32),
            pltpu.VMEM((rows, kv_dim), f32),
            pltpu.VMEM((n_swap, 2 * rows, SWAP_BLOCK, latent_dim), bf16),
            pltpu.VMEM((n_swap, 2 * rows, SWAP_BLOCK, rope_dim), bf16),
            pltpu.VMEM((rows, 1), f32),
            dma(()), dma((n_dq,)), dma(()), dma((n_uq,)), dma(()), dma((3,)), dma((3,)), dma((n_dq,)), dma((n_dq,)), dma(()), dma(()),
            dma((n_swap,)), dma((n_swap,)), dma((n_swap,)), dma((n_swap,)), dma((2, n_swap)),
        ],
        compiler_params=pltpu.CompilerParams(collective_id=1, has_side_effects=True, vmem_limit_bytes=66 * 1000 * 1000),
        name='front',
    )(hidden, norm_attn.reshape(1, -1), norm_q.reshape(-1, 128), norm_kv.reshape(1, -1), rope_cos.T, rope_sin.T,
      w_dq, w_dkv.T, jnp.transpose(w_uq, (1, 2, 0)).reshape(heads * head_dim, q_rank), w_uk)


def attention_rows(hidden, ckv_cache, kpe_cache, cache_len, rope_cos, rope_sin, norm_attn, w_dq, norm_q, w_uq, w_dkv, norm_kv, w_uk, w_uv):
    score_scale = MSCALE * MSCALE / math.sqrt(w_uq.shape[2])
    q_abs, q_pe, ckv_new, kpe_new = front(hidden, norm_attn, w_dq, norm_q, w_uq, w_dkv, norm_kv, w_uk, rope_cos, rope_sin)
    head_out, ckv_new, kpe_new = attend(q_abs, q_pe, ckv_new, kpe_new, ckv_cache, kpe_cache, cache_len, w_uv, score_scale)
    return head_out, ckv_new, kpe_new


def tail_kernel(o_ref, x_ref, gain_ref, wout_ref, wgate_ref, wup_ref, wdown_ref, out_ref,
                slots, o_chip, x_chip, x_own, r_all, u_all, gate_buf, up_buf, act, sq_acc, pair_send, pair_recv, far_send, far_recv, own_sum, out_buf,
                slot_sem, in_send, in_recv, loc_sem, rp_send, rp_recv, rx_send, rx_recv, rf_send, rf_recv,
                pp_send, pp_recv, px_send, px_recv, out_sem):
    rep, me, chip, core = _sides()
    part = chip * 2 + (1 - core)
    opp = (1 - chip) * 2 + core
    diag = (1 - chip) * 2 + (1 - core)
    attn_k = wout_ref.shape[0]
    d_model = wgate_ref.shape[0]
    ff = wgate_ref.shape[1]
    rows = x_ref.shape[0]
    half = d_model // 2
    n_out = half // OUT_W
    n_ff = ff // OUT_W
    n_down = d_model // OUT_W
    first_ff = n_out
    first_down = n_out + 2 * n_ff
    total = first_down + n_down
    pieces = OUT_W // PIECE
    n_half = half // PIECE
    n_all = d_model // PIECE

    def col(index):
        return pl.ds(pl.multiple_of(index * OUT_W, OUT_W), OUT_W)

    def piece(index):
        return pl.ds(pl.multiple_of(index * PIECE, PIECE), PIECE)

    def row_block(owner, count=1):
        return pl.ds(pl.multiple_of(owner * rows, rows), count * rows)

    def slot_copy(kind, index, step):
        slot = lax.rem(step, SLOTS)
        src = {'out': wout_ref, 'gate': wgate_ref, 'up': wup_ref, 'down': wdown_ref}[kind]
        depth = src.shape[0]
        return pltpu.make_async_copy(src.at[:, col(index)], slots.at[slot, pl.ds(0, depth), :], slot_sem.at[slot])

    def fetch(step):
        @pl.when(step < first_ff)
        def _():
            slot_copy('out', core * n_out + step, step).start()

        @pl.when((step >= first_ff) & (step < first_down) & (lax.rem(step - first_ff, 2) == 0))
        def _():
            slot_copy('gate', (step - first_ff) // 2, step).start()

        @pl.when((step >= first_ff) & (step < first_down) & (lax.rem(step - first_ff, 2) == 1))
        def _():
            slot_copy('up', (step - first_ff) // 2, step).start()

        @pl.when((step >= first_down) & (step < total))
        def _():
            slot_copy('down', step - first_down, step).start()

    my_rows = row_block(core)
    my_half = pl.ds(pl.multiple_of(core * half, half), half)
    their_half = pl.ds(pl.multiple_of((1 - core) * half, half), half)
    keep_o = pltpu.make_async_copy(o_ref, o_chip.at[my_rows, :], loc_sem.at[0])
    keep_x = pltpu.make_async_copy(x_ref.at[:, my_half], x_chip.at[my_rows, :], loc_sem.at[1])
    give_x = pltpu.make_async_copy(x_ref.at[:, their_half], x_own, loc_sem.at[2])
    keep_o.start()
    give_x.start()
    keep_x.start()
    slot_copy('out', core * n_out, 0).start()

    barrier = pltpu.get_barrier_semaphore()
    for peer in (part, opp):
        pl.semaphore_signal(barrier, inc=1, device_id=(rep, peer), device_id_type=MESH)
    pl.semaphore_wait(barrier, 2)

    def remote(src, dst, send, recv, peer):
        return pltpu.make_async_remote_copy(src_ref=src, dst_ref=dst, send_sem=send, recv_sem=recv,
                                            device_id=(rep, peer), device_id_type=MESH)

    keep_o.wait()
    send_o = remote(o_chip.at[my_rows, :], o_chip.at[my_rows, :], in_send.at[0], in_recv.at[0], part)
    send_o.start()
    give_x.wait()
    send_x = remote(x_own, x_chip.at[my_rows, :], in_send.at[1], in_recv.at[1], part)
    send_x.start()
    for step in range(1, SLOTS):
        slot_copy('out', core * n_out + step, step).start()
    sq_acc[...] = jnp.zeros_like(sq_acc)
    gate_buf[...] = jnp.zeros_like(gate_buf)
    up_buf[...] = jnp.zeros_like(up_buf)
    keep_x.wait()
    send_o.wait()
    send_x.wait()

    chip_rows = row_block(chip * 2, 2)
    far_rows = row_block((1 - chip) * 2, 2)

    def r_pair(index):
        blk = r_all.at[core * n_half + index, chip_rows, :]
        return remote(blk, blk, rp_send.at[index], rp_recv.at[index], part)

    def r_far(index):
        blk = r_all.at[core * n_half + index, chip_rows, :]
        return remote(blk, blk, rx_send.at[index], rx_recv.at[index], opp)

    def r_forward(index):
        blk = r_all.at[core * n_half + index, far_rows, :]
        return remote(blk, blk, rf_send.at[index], rf_recv.at[index], part)

    def add_squares(sel, vals):
        wide = vals.astype(jnp.float32)
        wide = wide * wide
        acc = sq_acc[sel, :]
        for lane in range(0, PIECE, 128):
            acc = acc + wide[:, lane:lane + 128]
        sq_acc[sel, :] = acc

    def take_pair(index):
        r_pair(index).wait_recv()
        add_squares(chip_rows, r_all[(1 - core) * n_half + index, chip_rows, :])

    def take_far(index):
        r_far(index).wait_recv()
        r_forward(index).start()
        add_squares(far_rows, r_all[core * n_half + index, far_rows, :])

    def take_forward(index):
        r_forward(index).wait_recv()
        add_squares(far_rows, r_all[(1 - core) * n_half + index, far_rows, :])

    lags = ((take_pair, 2), (take_far, 4), (take_forward, 6))

    def out_step(index, carry):
        slot_copy('out', core * n_out + index, index).wait()
        for sub in range(pieces):
            here = index * pieces + sub
            acc = jnp.dot(o_chip[...], slots[lax.rem(index, SLOTS), :attn_k, sub * PIECE:(sub + 1) * PIECE], preferred_element_type=jnp.float32)
            vals = (x_chip[:, piece(here)].astype(jnp.float32) + acc).astype(jnp.bfloat16)
            r_all[core * n_half + here, chip_rows, :] = vals
            r_far(here).start()
            r_pair(here).start()
            add_squares(chip_rows, vals)
            for take, lag in lags:
                @pl.when(here >= lag)
                def _(take=take, lag=lag):
                    take(here - lag)
        fetch(index + SLOTS)
        return carry

    lax.fori_loop(0, n_out, out_step, 0)

    def inverse(owner):
        total_sq = jnp.sum(sq_acc[row_block(owner), :], axis=-1, keepdims=True)
        return lax.rsqrt(total_sq * (1.0 / d_model) + EPSILON)

    def normalise(places):
        invs = [inverse(owner) for _, owner in places]

        def norm_step(index, carry):
            for (place, owner), inv in zip(places, carry):
                vals = r_all[index, row_block(owner), :].astype(jnp.float32) * inv * gain_ref[0:1, piece(index)]
                u_all[place * rows:(place + 1) * rows, piece(index)] = vals.astype(jnp.bfloat16)
            return carry

        lax.fori_loop(0, n_all, norm_step, tuple(invs))

    for index in range(n_half - 2, n_half):
        take_pair(index)
    take_far(n_half - 4)
    take_forward(n_half - 6)
    take_far(n_half - 3)
    take_forward(n_half - 5)
    normalise(((0, part), (1, me)))
    near = slice(0, 2 * rows)
    far = slice(2 * rows, 4 * rows)

    def activate(gate_val, up_val):
        return (gate_val * jax.nn.sigmoid(gate_val) * up_val).astype(jnp.bfloat16)

    def product(sel, step):
        return jnp.dot(u_all[sel, :], slots[lax.rem(step, SLOTS), :d_model, :], preferred_element_type=jnp.float32)

    def early(index, sel):
        step = first_ff + 2 * index
        gate_val = product(sel, step)
        act[sel, index * OUT_W:(index + 1) * OUT_W] = activate(gate_val, product(sel, step + 1))

    for index in range(EARLY):
        slot_copy('gate', index, first_ff + 2 * index).wait()
        slot_copy('up', index, first_ff + 2 * index + 1).wait()
        early(index, near)
        if index == 0:
            take_far(n_half - 2)
            take_far(n_half - 1)
            take_forward(n_half - 4)
            take_forward(n_half - 3)
    take_forward(n_half - 2)
    take_forward(n_half - 1)
    normalise(((2, diag), (3, opp)))
    for index in range(EARLY):
        early(index, far)
        fetch(first_ff + 2 * index + SLOTS)
        fetch(first_ff + 2 * index + 1 + SLOTS)

    def ff_step(index, carry):
        step = first_ff + 2 * index
        now, before = lax.rem(index, 2), lax.rem(index + 1, 2)
        slot_copy('gate', index, step).wait()
        act[:, col(jnp.maximum(index - 1, EARLY))] = activate(gate_buf[before], up_buf[...])
        gate_buf[now] = product(slice(None), step)
        fetch(step + SLOTS)
        slot_copy('up', index, step + 1).wait()
        up_buf[...] = product(slice(None), step + 1)
        fetch(step + 1 + SLOTS)
        return carry

    lax.fori_loop(EARLY, n_ff, ff_step, 0)
    act[:, (n_ff - 1) * OUT_W:] = activate(gate_buf[(n_ff - 1) % 2], up_buf[...])

    def pair_copy(index):
        return remote(pair_send.at[index], pair_recv.at[index], pp_send.at[index], pp_recv.at[index], part)

    def far_copy(index):
        return remote(far_send.at[index], far_recv.at[index], px_send.at[index], px_recv.at[index], opp)

    def combine(index):
        pair_copy(index).wait_recv()
        far_send[index] += pair_recv[index, rows:, :]
        far_copy(index).start()
        own_sum[index] += pair_recv[index, :rows, :]

    def down_step(index, carry):
        step = first_down + index
        slot_copy('down', index, step).wait()
        for sub in range(pieces):
            here = index * pieces + sub
            part_sum = jnp.dot(act[...], slots[lax.rem(step, SLOTS), :ff, sub * PIECE:(sub + 1) * PIECE], preferred_element_type=jnp.float32)
            pair_send[here, :rows] = part_sum[:rows]
            pair_send[here, rows:] = part_sum[2 * rows:3 * rows]
            own_sum[here] = part_sum[rows:2 * rows]
            far_send[here] = part_sum[3 * rows:]
            pair_copy(here).start()

            @pl.when(here >= 1)
            def _():
                combine(here - 1)
        fetch(step + SLOTS)
        return carry

    lax.fori_loop(0, n_down, down_step, 0)
    combine(n_all - 1)

    def settle(index, carry):
        r_pair(index).wait_send()
        r_far(index).wait_send()
        r_forward(index).wait_send()
        return carry

    lax.fori_loop(0, n_half, settle, 0)
    own_rows = row_block(me)

    def out_copy(index):
        return pltpu.make_async_copy(out_buf.at[:, piece(index)], out_ref.at[:, piece(index)], out_sem.at[index])

    def finish(index, carry):
        far_copy(index).wait()
        pair_copy(index).wait_send()
        mlp = own_sum[index] + far_recv[index]
        out_buf[:, piece(index)] = (r_all[index, own_rows, :].astype(jnp.float32) + mlp).astype(jnp.bfloat16)
        out_copy(index).start()
        return carry

    lax.fori_loop(0, n_all, finish, 0)

    def flush(index, carry):
        out_copy(index).wait()
        return carry

    lax.fori_loop(0, n_all, flush, 0)


def tail(head_out, hidden, norm_mlp, w_out, w_gate, w_up, w_down):
    rows, d_model = hidden.shape
    attn_k = w_out.shape[0]
    ff = w_gate.shape[1]
    n_half = d_model // 2 // PIECE
    n_all = d_model // PIECE
    depth = max(attn_k, d_model, ff)
    vmem = pl.BlockSpec(memory_space=pltpu.VMEM)
    anywhere = pl.BlockSpec(memory_space=pl.ANY)
    dma = pltpu.SemaphoreType.DMA
    f32, bf16 = jnp.float32, jnp.bfloat16
    return pl.pallas_call(
        tail_kernel,
        out_shape=jax.ShapeDtypeStruct((rows, d_model), bf16),
        in_specs=[anywhere, anywhere, vmem, anywhere, anywhere, anywhere, anywhere],
        out_specs=anywhere,
        scratch_shapes=[
            pltpu.VMEM((SLOTS, depth, OUT_W), bf16),
            pltpu.VMEM((2 * rows, attn_k), bf16),
            pltpu.VMEM((2 * rows, d_model // 2), bf16),
            pltpu.VMEM((rows, d_model // 2), bf16),
            pltpu.VMEM((n_all, 4 * rows, PIECE), bf16),
            pltpu.VMEM((4 * rows, d_model), bf16),
            pltpu.VMEM((2, 4 * rows, OUT_W), f32),
            pltpu.VMEM((4 * rows, OUT_W), f32),
            pltpu.VMEM((4 * rows, ff), bf16),
            pltpu.VMEM((4 * rows, 128), f32),
            pltpu.VMEM((n_all, 2 * rows, PIECE), f32),
            pltpu.VMEM((n_all, 2 * rows, PIECE), f32),
            pltpu.VMEM((n_all, rows, PIECE), f32),
            pltpu.VMEM((n_all, rows, PIECE), f32),
            pltpu.VMEM((n_all, rows, PIECE), f32),
            pltpu.VMEM((rows, d_model), bf16),
            dma((SLOTS,)), dma((2,)), dma((2,)), dma((3,)),
            dma((n_half,)), dma((n_half,)), dma((n_half,)), dma((n_half,)), dma((n_half,)), dma((n_half,)),
            dma((n_all,)), dma((n_all,)), dma((n_all,)), dma((n_all,)), dma((n_all,)),
        ],
        compiler_params=pltpu.CompilerParams(collective_id=0, has_side_effects=True, vmem_limit_bytes=66 * 1000 * 1000),
        name='tail',
    )(head_out, hidden, norm_mlp.reshape(1, d_model), w_out, w_gate, w_up, w_down)


def solution(mesh):
    row_spec = P(('rep', 'dp'), None)
    cube_spec = P(('rep', 'dp'), None, None)
    full_spec = P()
    in_specs = (row_spec, cube_spec, cube_spec, P(('rep', 'dp')), row_spec, row_spec,
                full_spec, full_spec, full_spec, full_spec, full_spec, full_spec, full_spec, full_spec, full_spec, full_spec,
                P(None, 'dp'), P(None, 'dp'), P('dp', None))

    def local_step(hidden, ckv_cache, kpe_cache, cache_len, rope_cos, rope_sin, norm_attn, w_dq, norm_q, w_uq, w_dkv, norm_kv, w_uk, w_uv, w_out, norm_mlp, w_gate, w_up, w_down):
        head_out, ckv_new, kpe_new = attention_rows(hidden, ckv_cache, kpe_cache, cache_len, rope_cos, rope_sin, norm_attn, w_dq, norm_q, w_uq, w_dkv, norm_kv, w_uk, w_uv)
        out_hidden = tail(head_out, hidden, norm_mlp, w_out.reshape(-1, w_out.shape[-1]), w_gate, w_up, w_down)
        return out_hidden, ckv_new, kpe_new

    return jax.shard_map(local_step, mesh=mesh, in_specs=in_specs, out_specs=(row_spec, row_spec, row_spec), check_vma=False)
```
